512 devices in a mesh: gx: 4 (over x), gy: 16 (over z_hi, y), gz: 8 (over z_lo, core).
Axes of the slice: x: 4, y: 8, z: 8 (z_hi: 2, z_lo: 4; z = z_hi * 4 + z_lo), core: 2. Of those that a mesh axis runs over, the one named last changes fastest.
Arguments:
- displacement: bfloat16 [16, 16, 16, 12, 3, 32, 128], P('gx', 'gy', 'gz'), may hold values from -96 to 96
- dof_weight: bfloat16 [16, 16, 16, 12, 128], P('gx', 'gy', 'gz'), may hold values from 0.099609375 to 10
- coarse_matrix: float32 [16, 16, 16, 27, 36, 36], P('gx', 'gy', 'gz'), may hold values from -48 to 48, as said below
- block_inverse: float32 [16, 16, 16, 36, 36], P('gx', 'gy', 'gz'), may hold values from -12 to 12, as said below
Outputs:
- edge_average: float32 [16, 16, 16, 12, 3, 32], P('gx', 'gy', 'gz')
- coarse_solution: float32 [16, 16, 16, 36, 32], P('gx', 'gy', 'gz')
The draws below stay inside these ranges and needn't reach their ends.
Inputs may be any that keep to these rules, and one draw needn't show every extreme that they name: coarse_matrix is the replicated form of one operator over edge unknowns: rows of the same edge seen from its four subdomains are equal, and each column of an edge is stored at exactly one of that edge's subdomains (zeros at the others). block_inverse[p] is block-diagonal in 3 x 3 blocks, each the inverse of the matching diagonal 3 x 3 block of coarse_matrix[p, 13].
All inputs are finite; a program needn't handle non-finite values.
Results may differ from the reference program's by a relative error of at most 0.0003.
Values sent between devices are 32-bit elements; how exact they have to be, the bound alone decides.
No kernel may reach another device: no remote copies, remote signals or barrier semaphores. Data moves between devices by JAX's collectives and lax.ppermute only.
A program may use at most 64 MiB of HBM per device.

```python
import math
import jax
import jax.numpy as jnp
import numpy as np
from jax import lax

RHS = 32
EDGES = 12
COMP = 3
DOFS = 128
SWEEPS = 4
COARSE = 36
NX = 16
NY = 16
NZ = 16


edge_offsets = np.array([[0, 0, 0], [0, 0, 1], [0, 1, 0], [0, 1, 1], [0, 0, 0], [0, 0, 1], [1, 0, 0], [1, 0, 1], [0, 0, 0], [0, 1, 0], [1, 0, 0], [1, 1, 0]])


def owner_mask():
    table = np.zeros((27, 9, 9), np.float32)
    for offset in range(27):
        delta = [offset // 9 - 1, offset // 3 % 3 - 1, offset % 3 - 1]
        for row_dir in range(3):
            for col_dir in range(3):
                if row_dir == col_dir or delta[col_dir] <= 0:
                    table[offset, 3 * row_dir:3 * row_dir + 3, 3 * col_dir:3 * col_dir + 3] = 1.0
    return table


def placement_table():
    table = np.full((12, 27, 12), 81, np.int32)
    for edge in range(12):
        row_dir = edge // 4
        anchor = edge_offsets[edge]
        for offset in range(27):
            delta = [offset // 9 - 1, offset // 3 % 3 - 1, offset % 3 - 1]
            for col_dir in range(3):
                if not (row_dir == col_dir or delta[col_dir] <= 0):
                    continue
                target = []
                for comp in range(3):
                    if comp == col_dir:
                        target.append(0)
                    else:
                        target.append(1 if anchor[comp] + delta[comp] >= 1 else 0)
                other = -1
                for cand in range(4 * col_dir, 4 * col_dir + 4):
                    if list(edge_offsets[cand]) == target:
                        other = cand
                place = [anchor[comp] + delta[comp] - target[comp] for comp in range(3)]
                stored = 9 * (place[0] + 1) + 3 * (place[1] + 1) + (place[2] + 1)
                table[edge, stored, other] = 3 * offset + col_dir
    return table


def coarse_pair(key):
    base_key = jax.random.fold_in(key, 7)
    noise_key, scale_key = jax.random.split(base_key)
    noise = jax.random.normal(noise_key, (NX, NY, NZ, 27, 9, 9), jnp.float32) * 0.03
    noise = noise * jnp.asarray(owner_mask())
    blocks = noise.at[:, :, :, 13].add(2.0 * jnp.eye(9, dtype=jnp.float32))
    spread = math.log(2.0)
    scales = jnp.exp(jax.random.uniform(scale_key, (NX, NY, NZ, 9), jnp.float32, -spread, spread))
    column_list = []
    for offset in range(27):
        shift_x = offset // 9 - 1
        shift_y = offset // 3 % 3 - 1
        shift_z = offset % 3 - 1
        column_list.append(jnp.roll(scales, (-shift_x, -shift_y, -shift_z), (0, 1, 2)))
    columns = jnp.stack(column_list, 3)
    owned = scales[:, :, :, None, :, None] * blocks * columns[:, :, :, :, None, :]
    diag_list = []
    for direction in range(3):
        diag_list.append(jnp.linalg.inv(owned[:, :, :, 13, 3 * direction:3 * direction + 3, 3 * direction:3 * direction + 3]))
    diag_inverse = jnp.stack(diag_list, 3)
    table = placement_table()
    row_blocks = []
    inverse_blocks = []
    for edge in range(12):
        row_dir = edge // 4
        anchor = edge_offsets[edge]
        rolled = jnp.roll(owned, (-int(anchor[0]), -int(anchor[1]), -int(anchor[2])), (0, 1, 2))
        rows = rolled[:, :, :, :, 3 * row_dir:3 * row_dir + 3, :]
        rows = rows.reshape(NX, NY, NZ, 27, 3, 3, 3)
        rows = jnp.transpose(rows, (0, 1, 2, 3, 5, 4, 6)).reshape(NX, NY, NZ, 81, 3, 3)
        rows = jnp.concatenate([rows, jnp.zeros((NX, NY, NZ, 1, 3, 3), jnp.float32)], 3)
        picked = jnp.take(rows, jnp.asarray(table[edge]).reshape(-1), axis=3)
        picked = picked.reshape(NX, NY, NZ, 27, 12, 3, 3)
        picked = jnp.transpose(picked, (0, 1, 2, 3, 5, 4, 6)).reshape(NX, NY, NZ, 27, 3, 36)
        row_blocks.append(picked)
        rolled_inverse = jnp.roll(diag_inverse, (-int(anchor[0]), -int(anchor[1]), -int(anchor[2])), (0, 1, 2))
        inverse_blocks.append(rolled_inverse[:, :, :, row_dir])
    matrix = jnp.stack(row_blocks, 4).reshape(NX, NY, NZ, 27, 36, 36)
    stacked = jnp.stack(inverse_blocks, 3)
    inverse = jnp.einsum('xyzeab,ef->xyzeafb', stacked, jnp.eye(12, dtype=jnp.float32)).reshape(NX, NY, NZ, 36, 36)
    return (matrix, inverse)


def draw_coarse_matrix(key, part):
    return coarse_pair(key)[0]


def draw_block_inverse(key, part):
    return coarse_pair(key)[1]


def level_of(key, extent, shards, low, largest):
    def one(position, blocks):
        steps = jax.random.uniform(jax.random.fold_in(jax.random.fold_in(key, 6), position), (blocks,), jnp.float32, low / len(shards), largest / len(shards))
        return jnp.repeat(jnp.exp(steps), extent[position] // blocks).reshape((-1,) + (1,) * (len(extent) - position - 1))

    factor_of = one(*shards[0])
    for cut in shards[1:]:
        factor_of = factor_of * one(*cut)
    return factor_of


def centred(stream_key, shape, scale, limit, pieces=(), kind=jnp.bfloat16):
    entries = jax.random.normal(stream_key, shape, jnp.float32) * scale
    if len(pieces) > 0:
        entries = level_of(stream_key, shape, pieces, -0.22, 0.18) * entries
    return jnp.clip(entries, min=-limit, max=limit).astype(kind)


def setup_inputs(seed: int = 0) -> dict:
    streams_of = jax.random.split(jax.random.key(seed), 5)
    return {
        "displacement": centred(streams_of[0], (NX, NY, NZ, EDGES, COMP, RHS, DOFS), 16.0, 96.0, ((0, 4), (1, 16), (2, 8))),
        "dof_weight": jnp.clip(jnp.exp(math.log(10.0) - 4.609084 * jax.random.uniform(streams_of[1], (NX, NY, NZ, EDGES, DOFS), jnp.float32) ** level_of(streams_of[1], (NX, NY, NZ, EDGES, DOFS), ((0, 4), (1, 16), (2, 8)), -0.2, 0.2)), 0.099609375, 10.0).astype(jnp.bfloat16),
        "coarse_matrix": draw_coarse_matrix(jax.random.fold_in(streams_of[4], 71), 0),
        "block_inverse": draw_block_inverse(jax.random.fold_in(streams_of[4], 71), 0),
    }


edge_offsets = np.array([[0, 0, 0], [0, 0, 1], [0, 1, 0], [0, 1, 1], [0, 0, 0], [0, 0, 1], [1, 0, 0], [1, 0, 1], [0, 0, 0], [0, 1, 0], [1, 0, 0], [1, 1, 0]])

def combine(padded_numer, padded_weight, size_x, size_y, size_z):
    numer_list = []
    weight_list = []
    for edge in range(12):
        first = 4 * (edge // 4)
        numer_total = 0.0
        weight_total = 0.0
        for other in range(first, first + 4):
            delta = edge_offsets[edge] - edge_offsets[other]
            start_x = 1 + int(delta[0])
            start_y = 1 + int(delta[1])
            start_z = 1 + int(delta[2])
            numer_total = numer_total + padded_numer[start_x:start_x + size_x, start_y:start_y + size_y, start_z:start_z + size_z, other]
            weight_total = weight_total + padded_weight[start_x:start_x + size_x, start_y:start_y + size_y, start_z:start_z + size_z, other]
        numer_list.append(numer_total)
        weight_list.append(weight_total)
    return jnp.stack(numer_list, 3) / jnp.stack(weight_list, 3)[..., None, None]

def apply_matrix(padded, coarse_matrix, size_x, size_y, size_z):
    total = jnp.zeros((size_x, size_y, size_z) + padded.shape[3:], jnp.float32)
    for offset in range(27):
        start_x = offset // 9
        start_y = offset // 3 % 3
        start_z = offset % 3
        piece = padded[start_x:start_x + size_x, start_y:start_y + size_y, start_z:start_z + size_z]
        total = total + jnp.einsum('xyzij,xyzjr->xyzir', coarse_matrix[:, :, :, offset], piece, precision=lax.Precision.HIGHEST)
    return total

def reference(displacement, dof_weight, coarse_matrix, block_inverse):
    size_x, size_y, size_z = (displacement.shape[0], displacement.shape[1], displacement.shape[2])
    numers = jnp.einsum('xyzecrk,xyzek->xyzecr', displacement.astype(jnp.float32), dof_weight.astype(jnp.float32))
    weights = jnp.sum(dof_weight.astype(jnp.float32), axis=-1)
    padded_numer = jnp.pad(numers, ((1, 1), (1, 1), (1, 1), (0, 0), (0, 0), (0, 0)), mode='wrap')
    padded_weight = jnp.pad(weights, ((1, 1), (1, 1), (1, 1), (0, 0)), mode='wrap')
    averages = combine(padded_numer, padded_weight, size_x, size_y, size_z)
    rhs_rows = averages.reshape(size_x, size_y, size_z, COARSE, averages.shape[-1])
    iterate = jnp.einsum('xyzij,xyzjr->xyzir', block_inverse, rhs_rows, precision=lax.Precision.HIGHEST)
    for sweep in range(SWEEPS - 1):
        padded = jnp.pad(iterate, ((1, 1), (1, 1), (1, 1), (0, 0), (0, 0)), mode='wrap')
        product = apply_matrix(padded, coarse_matrix, size_x, size_y, size_z)
        iterate = iterate + jnp.einsum('xyzij,xyzjr->xyzir', block_inverse, rhs_rows - product, precision=lax.Precision.HIGHEST)
    return (averages, iterate)
```

```python
import functools

import jax
import jax.numpy as jnp
import numpy as np
from jax import lax
from jax.experimental import pallas as pl
from jax.experimental.pallas import tpu as pltpu
from jax.sharding import PartitionSpec as P

F32 = jnp.float32
BF16 = jnp.bfloat16
OFFSETS = (
    (0, 0, 0), (0, 0, 1), (0, 1, 0), (0, 1, 1),
    (0, 0, 0), (0, 0, 1), (1, 0, 0), (1, 0, 1),
    (0, 0, 0), (0, 1, 0), (1, 0, 0), (1, 1, 0),
)
SLOT_EDGES = (0, 2, 4, 8, 9)


def slot_of(edge):
    direction = edge // 4
    upper = OFFSETS[edge][1]
    return (0 + upper, 2, 3 + upper)[direction]


def placement():
    table = np.zeros((1024, 768), np.float32)
    for offset in range(27):
        dx, dy, dz = offset // 9 - 1, offset // 3 % 3 - 1, offset % 3 - 1
        for edge in range(12):
            ox, oy, oz = OFFSETS[edge]
            direction = edge // 4
            if direction == 1:
                group, slot = {-1: (1, 2), 0: (0, 2), 1: (2, 2)}[dy + oy]
            else:
                base = 0 if direction == 0 else 3
                group, slot = {-1: (1, base), 0: (0, base), 1: (0, base + 1), 2: (2, base + 1)}[dy + oy]
            for comp in range(3):
                row = 16 * group + 3 * slot + comp
                table[36 * offset + 3 * edge + comp, 192 * (dx + ox + 1) + 48 * (dz + oz + 1) + row] = 1.0
    return table


def shifted(block, axis, distance):
    count = lax.axis_size(axis)
    return lax.ppermute(block, axis, [((i - distance) % count, i) for i in range(count)])


def lanes(shape):
    return lax.broadcasted_iota(jnp.int32, shape, len(shape) - 1)


def split(value):
    high = value.astype(BF16)
    return high, (value - high.astype(F32)).astype(BF16)


def dot(a, b):
    return jnp.dot(a, b, preferred_element_type=F32)


def own_lanes(value):
    group = lanes((40, 128)) // 32
    total = jnp.where(group == 0, value[0:40], 0.0)
    for x in range(1, 4):
        total = total + jnp.where(group == x, value[40 * x : 40 * x + 40], 0.0)
    return total


def call(kernel, outs, scratch=(), flops=1_000_000, **options):
    return pl.pallas_call(
        kernel,
        out_shape=outs,
        scratch_shapes=list(scratch),
        cost_estimate=pl.CostEstimate(flops=flops, bytes_accessed=1_000_000, transcendentals=0),
        compiler_params=pltpu.CompilerParams(vmem_limit_bytes=40 * 1024 * 1024),
        **options,
    )


def shape(*dims, dtype=F32):
    return jax.ShapeDtypeStruct(dims, dtype)


def numer_kernel(disp_ref, weight_ref, sums_ref, moving_ref):
    ones = jnp.ones((128, 128), BF16)
    group = (lanes((4, 512)) % 128) // 32
    keep = group == lax.broadcasted_iota(jnp.int32, (4, 512), 0)
    for edge in range(12):
        for z in range(2):
            parts = [disp_ref[x, z, edge, c] for c in range(3) for x in range(4)]
            right = jnp.concatenate(parts + [ones], axis=0)
            left = weight_ref[edge, z]
            found = lax.dot_general(left, right, (((1,), (1,)), ((), ())), preferred_element_type=F32)
            row = jnp.sum(jnp.where(keep, found, 0.0), axis=0, keepdims=True)
            for c in range(4):
                piece = row[:, 128 * c : 128 * c + 128]
                sums_ref[z, 4 * edge + c : 4 * edge + c + 1, :] = piece
                if edge in (6, 7, 10, 11):
                    place = 4 * (6, 7, 10, 11).index(edge) + c
                    moving_ref[z, place : place + 1, :] = piece


def sum_x_kernel(sums_ref, moving_ref, left_ref, out_ref, up_ref):
    for z in range(2):
        last = lanes((16, 128)) >= 96
        below = pltpu.roll(jnp.where(last, left_ref[z], moving_ref[z]), 32, 1)
        out_ref[z, 0:16] = sums_ref[z, 0:16]
        out_ref[z, 16:24] = sums_ref[z, 16:24] + below[0:8]
        out_ref[z, 24:32] = sums_ref[z, 32:40] + below[8:16]
    up_ref[...] = out_ref[1, 0:24]


def sum_z_kernel(sums_ref, left_ref, lower_ref, upper_ref, middle_ref):
    for z in range(2):
        below = left_ref if z == 0 else sums_ref.at[0]
        lower_ref[z, 0:4] = sums_ref[z, 0:4] + below[4:8]
        lower_ref[z, 4:8] = sums_ref[z, 24:28]
        upper_ref[z, 0:4] = sums_ref[z, 8:12] + below[12:16]
        upper_ref[z, 4:8] = sums_ref[z, 28:32]
        middle_ref[z, 0:4] = sums_ref[z, 16:20] + below[20:24]
        middle_ref[z, 4:8] = sums_ref[z, 16:20]


def solve(block_high, block_low, rows_ref):
    high, low = split(rows_ref[...])
    found = dot(block_high, high) + dot(block_high, low) + dot(block_low, high)
    return own_lanes(found)


def first_kernel(lower_ref, upper_ref, middle_ref, below_ref, above_ref, bh_ref, bl_ref, out_ref, x_ref, rows, found):
    for z in range(2):
        rows[...] = jnp.zeros((48, 128), F32)
        out_ref[z] = jnp.zeros((32, 128), F32)
        x_ref[z] = jnp.zeros((16, 128), F32)
        node = lower_ref[z] + below_ref[z]
        top = upper_ref[z] + above_ref[z]
        middle = middle_ref[z]
        for slot, (source, at) in enumerate(((node, 0), (top, 0), (middle, 0), (node, 4), (top, 4))):
            average = source[at : at + 3] / source[at + 3 : at + 4]
            edge = SLOT_EDGES[slot]
            rows[3 * edge : 3 * edge + 3] = average
            out_ref[z, 16 + 3 * slot : 19 + 3 * slot] = average
        found[...] = solve(bh_ref[z, :, 0:48], bl_ref[z, :, 0:48], rows)
        for slot, edge in enumerate(SLOT_EDGES):
            value = found[3 * edge : 3 * edge + 3]
            out_ref[z, 3 * slot : 3 * slot + 3] = value
            x_ref[z, 3 * slot : 3 * slot + 3] = value


def prepare_kernel(matrix_ref, block_ref, place_ref, ah_ref, al_ref, bh_ref, bl_ref, packed, stacked):
    packed[7] = jnp.zeros((72, 128), F32)
    for offset in range(27):
        start, tile = 36 * offset % 128, 36 * offset // 128
        size = min(36, 128 - start)
        packed[tile, :, start : start + size] = matrix_ref[0, offset, :, 0:size]
        if size < 36:
            packed[tile + 1, :, 0 : 36 - size] = matrix_ref[0, offset, :, size:36]
    for z in range(2):
        high, low = split(jnp.concatenate([packed[k, pl.ds(z, 36, stride=2), :] for k in range(8)], axis=1))
        pad = jnp.zeros((4, 1024), BF16)
        stacked[40 * z : 40 * z + 40] = jnp.concatenate([high, pad], axis=0)
        stacked[80 + 40 * z : 120 + 40 * z] = jnp.concatenate([low, pad], axis=0)
    found = dot(stacked[...], place_ref[...]).astype(BF16)
    for z in range(2):
        ah_ref[z, 0] = found[40 * z : 40 * z + 40]
        al_ref[z, 0] = found[80 + 40 * z : 120 + 40 * z]
    packed[0] = jnp.zeros((72, 128), F32)
    packed[0, :, 0:36] = block_ref[0]
    for z in range(2):
        high, low = split(packed[0, pl.ds(z, 36, stride=2), :])
        pad = jnp.zeros((4, 128), BF16)
        bh_ref[z, 0] = jnp.concatenate([high, pad], axis=0)
        bl_ref[z, 0] = jnp.concatenate([low, pad], axis=0)


def prepare(matrix, block):
    table = jnp.asarray(placement(), BF16)
    outs = (shape(2, 4, 40, 768, dtype=BF16),) * 2 + (shape(2, 4, 40, 128, dtype=BF16),) * 2
    wide = pl.BlockSpec((2, 1, 40, 768), lambda i: (0, i, 0, 0))
    slim = pl.BlockSpec((2, 1, 40, 128), lambda i: (0, i, 0, 0))
    ah, al, bh, bl = call(
        prepare_kernel,
        outs,
        (pltpu.VMEM((8, 72, 128), F32), pltpu.VMEM((160, 1024), BF16)),
        flops=20_000_000,
        grid=(4,),
        in_specs=[
            pl.BlockSpec((1, 27, 72, 36), lambda i: (i, 0, 0, 0)),
            pl.BlockSpec((1, 72, 36), lambda i: (i, 0, 0)),
            pl.BlockSpec((1024, 768), lambda i: (0, 0)),
        ],
        out_specs=(wide, wide, slim, slim),
    )(matrix, block, table)
    return (
        ah.reshape(2, 160, 768), al.reshape(2, 160, 768),
        bh.reshape(2, 160, 128), bl.reshape(2, 160, 128),
    )


def views(near, far):
    lane = lanes(near.shape)
    return (
        pltpu.roll(jnp.where(lane >= 96, far, near), 32, 1),
        near,
        pltpu.roll(jnp.where(lane < 32, far, near), 96, 1),
        pltpu.roll(jnp.where(lane < 64, far, near), 64, 1),
    )


def product(high, low, kh_ref, kl_ref, z):
    kept = jnp.concatenate([h[48 * z : 48 * z + 192] for h in high], axis=0)
    rest = jnp.concatenate([h[48 * z : 48 * z + 192] for h in low], axis=0)
    both = dot(kh_ref[z], jnp.concatenate([kept, rest], axis=1))
    return own_lanes(both[:, 0:128] + both[:, 128:256] + dot(kl_ref[z], kept))


def gathered(own_ref, left_ref, right_ref):
    near = jnp.concatenate(
        [left_ref[:, 0:128], own_ref[0, :, 0:128], own_ref[1, :, 0:128], right_ref[0:96, 0:128]], axis=0
    )
    far = jnp.concatenate(
        [left_ref[:, 128:256], own_ref[0, :, 128:256], own_ref[1, :, 128:256], right_ref[0:96, 128:256]], axis=0
    )
    return views(near, far)


def sweep_kernel(own_ref, left_ref, right_ref, g_ref, ah_ref, al_ref, bh_ref, bl_ref, x_ref, rows, found):
    pairs = [split(view) for view in gathered(own_ref, left_ref, right_ref)]
    high, low = [p[0] for p in pairs], [p[1] for p in pairs]
    for z in range(2):
        found[...] = product(high, low, ah_ref, al_ref, z)
        rows[...] = jnp.zeros((48, 128), F32)
        for slot, edge in enumerate(SLOT_EDGES):
            rows[3 * edge : 3 * edge + 3] = g_ref[z, 3 * slot : 3 * slot + 3, 0:128] - found[3 * edge : 3 * edge + 3]
        found[...] = solve(bh_ref[z, :, 0:48], bl_ref[z, :, 0:48], rows)
        x_ref[z] = jnp.zeros((16, 128), F32)
        for slot, edge in enumerate(SLOT_EDGES):
            x_ref[z, 3 * slot : 3 * slot + 3] = (
                own_ref[z, 3 * slot : 3 * slot + 3, 0:128] + found[3 * edge : 3 * edge + 3]
            )


def average_kernel(g_ref, right_ref, wide_ref, out_ref, ahead):
    for z in range(3):
        source = g_ref.at[z] if z < 2 else right_ref.at[96:112]
        ahead[z, 0:16] = source[:, 0:128]
        ahead[z, 16:32] = views(source[:, 0:128], source[:, 128:256])[2]
    for z in range(2):
        wide_ref[z] = jnp.zeros((48, 128), F32)
        for edge in range(12):
            ox, _, oz = OFFSETS[edge]
            start = 16 * ox + 3 * slot_of(edge)
            value = ahead[z + oz, start : start + 3]
            wide_ref[z, 3 * edge : 3 * edge + 3] = value
        write(out_ref, z, wide_ref[z, 0:36])


def write(out_ref, z, value):
    for x in range(4):
        out_ref[x, z] = value[:, 32 * x : 32 * x + 32]


def last_kernel(own_ref, left_ref, right_ref, wide_ref, ah_ref, al_ref, bh_ref, bl_ref, out_ref, rows, ahead, state):
    seen = gathered(own_ref, left_ref, right_ref)
    pairs = [split(view) for view in seen]
    high, low = [p[0] for p in pairs], [p[1] for p in pairs]
    for z in range(3):
        ahead[z, 0:16] = seen[1][48 * z + 48 : 48 * z + 64]
        ahead[z, 16:32] = seen[2][48 * z + 48 : 48 * z + 64]
    for z in range(2):
        for edge in range(12):
            ox, _, oz = OFFSETS[edge]
            start = 16 * ox + 3 * slot_of(edge)
            state[3 * edge : 3 * edge + 3] = ahead[z + oz, start : start + 3]
        rows[...] = jnp.zeros((48, 128), F32)
        rows[0:36] = wide_ref[z, 0:36] - product(high, low, ah_ref, al_ref, z)[0:36]
        write(out_ref, z, state[0:36] + solve(bh_ref[z, :, 0:48], bl_ref[z, :, 0:48], rows)[0:36])


def body(displacement, dof_weight, coarse_matrix, block_inverse):
    lane = lanes((2, 16, 128))
    weights = jnp.transpose(dof_weight[:, 0], (2, 1, 0, 3))
    sums, moving = call(numer_kernel, (shape(2, 48, 128), shape(2, 16, 128)), flops=20_000_000)(
        displacement[:, 0], weights
    )
    matrix = jnp.transpose(coarse_matrix[:, 0], (0, 2, 3, 1, 4)).reshape(4, 27, 72, 36)
    block = jnp.transpose(block_inverse[:, 0], (0, 2, 1, 3)).reshape(4, 72, 36)
    ah, al, bh, bl = prepare(matrix, block)
    left = shifted(moving, "gx", 1)
    sums, up = call(sum_x_kernel, (shape(2, 32, 128), shape(24, 128)))(sums, moving, left)
    left = shifted(up, "gz", 1)
    lower, upper, middle = call(sum_z_kernel, (shape(2, 8, 128),) * 3)(sums, left)
    below, above = shifted(upper, "gy", 1), shifted(lower, "gy", -1)
    both, x = call(
        first_kernel,
        (shape(2, 32, 128), shape(2, 16, 128)),
        (pltpu.VMEM((48, 128), F32), pltpu.VMEM((40, 128), F32)),
    )(lower, upper, middle, below, above, bh, bl)
    average = None
    for sweep in range(3):
        left = shifted(x, "gx", 1)
        right = shifted(both if sweep == 0 else x, "gx", -1)
        x = jnp.concatenate([x, jnp.where(lane < 64, right[:, 0:16], left)], axis=2)
        if sweep == 0:
            g = jnp.concatenate([both[:, 16:32], right[:, 16:32]], axis=2)
        below, above = shifted(x, "gy", 1), shifted(x, "gy", -1)
        own = jnp.concatenate([x, below, above], axis=1)
        left = shifted(own[1], "gz", 1)
        moving = own.reshape(96, 256)
        if sweep == 0:
            moving = jnp.concatenate([moving, g[0]], axis=0)
        right = shifted(moving, "gz", -1)
        if sweep == 0:
            wide, average = call(
                average_kernel, (shape(2, 48, 128), shape(4, 2, 36, 32)), (pltpu.VMEM((3, 32, 128), F32),)
            )(g, right)
        small = (pltpu.VMEM((48, 128), F32), pltpu.VMEM((40, 128), F32))
        if sweep < 2:
            x = call(sweep_kernel, shape(2, 16, 128), small, flops=10_000_000)(
                own, left, right, g, ah, al, bh, bl
            )
        else:
            x = call(
                last_kernel,
                shape(4, 2, 36, 32),
                (pltpu.VMEM((48, 128), F32), pltpu.VMEM((3, 32, 128), F32), pltpu.VMEM((40, 128), F32)),
                flops=10_000_000,
            )(own, left, right, wide, ah, al, bh, bl)
    return average.reshape(4, 1, 2, 12, 3, 32), x.reshape(4, 1, 2, 36, 32)


def solution(mesh):
    placed = (
        P("gx", "gy", "gz", None, None, None, None),
        P("gx", "gy", "gz", None, None),
        P("gx", "gy", "gz", None, None, None),
        P("gx", "gy", "gz", None, None),
    )
    return jax.shard_map(
        body,
        mesh=mesh,
        in_specs=placed,
        out_specs=(P("gx", "gy", "gz", None, None, None), P("gx", "gy", "gz", None, None)),
        check_vma=False,
    )
```

```python
import functools

import jax
import jax.numpy as jnp
import numpy as np
from jax import lax
from jax.experimental import pallas as pl
from jax.experimental.pallas import tpu as pltpu
from jax.sharding import PartitionSpec as P

F32 = jnp.float32
BF16 = jnp.bfloat16
OFFSETS = (
    (0, 0, 0), (0, 0, 1), (0, 1, 0), (0, 1, 1),
    (0, 0, 0), (0, 0, 1), (1, 0, 0), (1, 0, 1),
    (0, 0, 0), (0, 1, 0), (1, 0, 0), (1, 1, 0),
)
SLOT_EDGES = (0, 2, 4, 8, 9)
WIDE_EDGES = (0, 2, 4, 8, 9, 6, 10, 11)


def slot_of(edge):
    direction = edge // 4
    upper = OFFSETS[edge][1]
    return (0 + upper, 2, 3 + upper)[direction]


def placement():
    table = np.zeros((1024, 768), np.float32)
    for offset in range(27):
        dx, dy, dz = offset // 9 - 1, offset // 3 % 3 - 1, offset % 3 - 1
        for edge in range(12):
            ox, oy, oz = OFFSETS[edge]
            direction = edge // 4
            if direction == 1:
                group, slot = {-1: (1, 2), 0: (0, 2), 1: (2, 2)}[dy + oy]
            else:
                base = 0 if direction == 0 else 3
                group, slot = {-1: (1, base), 0: (0, base), 1: (0, base + 1), 2: (2, base + 1)}[dy + oy]
            for comp in range(3):
                row = 16 * group + 3 * slot + comp
                table[36 * offset + 3 * edge + comp, 192 * (dx + ox + 1) + 48 * (dz + oz + 1) + row] = 1.0
    return table


def choice():
    table = np.zeros((128, 128), np.float32)
    for place, edge in enumerate(WIDE_EDGES):
        for comp in range(3):
            table[3 * edge + comp, 3 * place + comp] = 1.0
    return table


def shifted(block, axis, distance):
    count = lax.axis_size(axis)
    return lax.ppermute(block, axis, [((i - distance) % count, i) for i in range(count)])


def lanes(shape):
    return lax.broadcasted_iota(jnp.int32, shape, len(shape) - 1)


def split(value):
    high = value.astype(BF16)
    return high, (value - high.astype(F32)).astype(BF16)


def dot(a, b):
    return jnp.dot(a, b, preferred_element_type=F32)


def own_lanes(value):
    group = lanes((40, 128)) // 32
    total = jnp.where(group == 0, value[0:40], 0.0)
    for x in range(1, 4):
        total = total + jnp.where(group == x, value[40 * x : 40 * x + 40], 0.0)
    return total


def call(kernel, outs, scratch=(), flops=1_000_000, **options):
    return pl.pallas_call(
        kernel,
        out_shape=outs,
        scratch_shapes=list(scratch),
        cost_estimate=pl.CostEstimate(flops=flops, bytes_accessed=1_000_000, transcendentals=0),
        compiler_params=pltpu.CompilerParams(vmem_limit_bytes=40 * 1024 * 1024),
        **options,
    )


def shape(*dims, dtype=F32):
    return jax.ShapeDtypeStruct(dims, dtype)


def numer_kernel(disp_ref, weight_ref, sums_ref):
    ones = jnp.ones((128, 128), BF16)
    group = (lanes((4, 512)) % 128) // 32
    keep = group == lax.broadcasted_iota(jnp.int32, (4, 512), 0)
    for edge in range(12):
        for z in range(2):
            parts = [disp_ref[x, z, edge, c] for c in range(3) for x in range(4)]
            right = jnp.concatenate(parts + [ones], axis=0)
            left = weight_ref[edge, z]
            found = lax.dot_general(left, right, (((1,), (1,)), ((), ())), preferred_element_type=F32)
            row = jnp.sum(jnp.where(keep, found, 0.0), axis=0, keepdims=True)
            for c in range(4):
                sums_ref[z, 4 * edge + c : 4 * edge + c + 1, :] = row[:, 128 * c : 128 * c + 128]


def sum_x_kernel(sums_ref, left_ref, right_ref, out_ref, up_ref):
    for z in range(2):
        all_x = jnp.concatenate([left_ref[z], sums_ref[z], right_ref[z]], axis=1)
        below = pltpu.roll(all_x, 32, 1)
        out_ref[z, 0:16] = all_x[0:16]
        out_ref[z, 16:24] = all_x[16:24] + below[24:32]
        out_ref[z, 24:32] = all_x[32:40] + below[40:48]
    up_ref[...] = out_ref[1, 0:24]


def sum_z_kernel(sums_ref, left_ref, lower_ref, upper_ref, middle_ref):
    for z in range(2):
        below = left_ref if z == 0 else sums_ref.at[0]
        lower_ref[z, 0:4] = sums_ref[z, 0:4] + below[4:8]
        lower_ref[z, 4:8] = sums_ref[z, 24:28]
        upper_ref[z, 0:4] = sums_ref[z, 8:12] + below[12:16]
        upper_ref[z, 4:8] = sums_ref[z, 28:32]
        middle_ref[z, 0:4] = sums_ref[z, 16:20] + below[20:24]
        middle_ref[z, 4:8] = sums_ref[z, 16:20]


def by_x(value, count, rows):
    group = lanes((rows, value.shape[1])) // 32
    total = jnp.where(group == 0, value[0:rows], 0.0)
    for x in range(1, count):
        total = total + jnp.where(group == x, value[rows * x : rows * x + rows], 0.0)
    return total


def three(high, low, value):
    kept, rest = split(value)
    return dot(high, kept) + dot(high, rest) + dot(low, kept)


def solve(block_high, block_low, rows_ref):
    return own_lanes(three(block_high, block_low, rows_ref[...]))


def first_kernel(lower_ref, upper_ref, middle_ref, below_ref, above_ref, bh_ref, bl_ref, g_ref, wide_ref, x_ref, rows):
    for z in range(2):
        rows[...] = jnp.zeros((32, 384), F32)
        node = lower_ref[z] + below_ref[z]
        top = upper_ref[z] + above_ref[z]
        middle = middle_ref[z]
        for slot, (source, at) in enumerate(((node, 0), (top, 0), (middle, 0), (node, 4), (top, 4))):
            rows[3 * slot : 3 * slot + 3] = source[at : at + 3] / source[at + 3 : at + 4]
        found = by_x(three(bh_ref[z, :, 0:32], bl_ref[z, :, 0:32], rows[...]), 12, 24)
        x_ref[z] = jnp.where(lax.broadcasted_iota(jnp.int32, (16, 384), 0) < 15, found[0:16], 0.0)
        g_ref[z] = rows[0:16]
        wide_ref[z, 0:16] = pltpu.roll(rows[0:16], 320, 1)[:, 0:256]
        wide_ref[z, 15:24] = pltpu.roll(rows[0:16], 288, 1)[6:15, 0:256]


def pick(rows_ref, value):
    rows_ref[...] = value
    return [rows_ref[3 * edge : 3 * edge + 3] for edge in WIDE_EDGES]


def prepare_kernel(
    matrix_ref, block_ref, place_ref, choice_ref, ah_ref, al_ref, bh_ref, bl_ref, out_ref, packed, stacked, full, small
):
    step = pl.program_id(0)
    packed[7] = jnp.zeros((72, 128), F32)
    for offset in range(27):
        start, tile = 36 * offset % 128, 36 * offset // 128
        size = min(36, 128 - start)
        packed[tile, :, start : start + size] = matrix_ref[0, offset, :, 0:size]
        if size < 36:
            packed[tile + 1, :, 0 : 36 - size] = matrix_ref[0, offset, :, size:36]
    for z in range(2):
        high, low = split(jnp.concatenate([packed[k, pl.ds(z, 36, stride=2), :] for k in range(8)], axis=1))
        pad = jnp.zeros((4, 1024), BF16)
        stacked[40 * z : 40 * z + 40] = jnp.concatenate([high, pad], axis=0)
        stacked[80 + 40 * z : 120 + 40 * z] = jnp.concatenate([low, pad], axis=0)
    found = dot(stacked[...], place_ref[...])
    for z in range(2):
        high, low = found[40 * z : 40 * z + 40], found[80 + 40 * z : 120 + 40 * z]
        ah_ref[z, 0] = high.astype(BF16)
        al_ref[z, 0] = low.astype(BF16)
        for place, value in enumerate(pick(full, high + low)):
            out_ref[0, z, 3 * place : 3 * place + 3, 0:768] = value
    for which in range(2):
        packed[0] = jnp.zeros((72, 128), F32)
        packed[0, :, 0:36] = block_ref[lax.rem(step + 2 * which, 4)]
        for z in range(2):
            high, low = split(packed[0, pl.ds(z, 36, stride=2), :])
            pad = jnp.zeros((4, 128), BF16)
            high, low = jnp.concatenate([high, pad], axis=0), jnp.concatenate([low, pad], axis=0)
            if which == 0:
                bh_ref[z, 0] = high
                bl_ref[z, 0] = low
            value = dot(high, choice_ref[...]) + dot(low, choice_ref[...])
            at = 768 + 128 * which
            for place, piece in enumerate(pick(small, value)):
                out_ref[0, z, 3 * place : 3 * place + 3, at : at + 128] = piece


def prepare(matrix, block):
    outs = (shape(2, 4, 40, 768, dtype=BF16),) * 2 + (shape(2, 4, 40, 128, dtype=BF16),) * 2
    outs = outs + (shape(4, 2, 24, 1024),)
    wide = pl.BlockSpec((2, 1, 40, 768), lambda i: (0, i, 0, 0))
    slim = pl.BlockSpec((2, 1, 40, 128), lambda i: (0, i, 0, 0))
    ah, al, bh, bl, sent = call(
        prepare_kernel,
        outs,
        (
            pltpu.VMEM((8, 72, 128), F32),
            pltpu.VMEM((160, 1024), BF16),
            pltpu.VMEM((40, 768), F32),
            pltpu.VMEM((40, 128), F32),
        ),
        flops=20_000_000,
        grid=(4,),
        in_specs=[
            pl.BlockSpec((1, 27, 72, 36), lambda i: (i, 0, 0, 0)),
            pl.BlockSpec((4, 72, 36), lambda i: (0, 0, 0)),
            pl.BlockSpec((1024, 768), lambda i: (0, 0)),
            pl.BlockSpec((128, 128), lambda i: (0, 0)),
        ],
        out_specs=(wide, wide, slim, slim, pl.BlockSpec((1, 2, 24, 1024), lambda i: (i, 0, 0, 0))),
    )(matrix, block, jnp.asarray(placement(), BF16), jnp.asarray(choice(), BF16))
    return (
        ah.reshape(2, 160, 768), al.reshape(2, 160, 768),
        bh.reshape(2, 160, 128), bl.reshape(2, 160, 128), sent,
    )


def merge_kernel(own_ref, left_ref, right_ref, ah_ref, al_ref, bh_ref, bl_ref):
    for z in range(2):
        cells = [left_ref.at[0, z], left_ref.at[1, z]] + [own_ref.at[x, z] for x in range(4)]
        cells = cells + [right_ref.at[0, z], right_ref.at[1, z]]
        ah_ref[z], al_ref[z] = split(jnp.concatenate([c[:, 0:768] for c in cells], axis=0))
        first, second = slice(768, 896), slice(896, 1024)
        parts = [c[:, second] for c in cells[0:2]] + [c[:, first] for c in cells] + [c[:, second] for c in cells[6:8]]
        bh_ref[z], bl_ref[z] = split(jnp.concatenate(parts, axis=0))


def views(near, far):
    lane = lanes(near.shape)
    return (
        pltpu.roll(jnp.where(lane >= 96, far, near), 32, 1),
        near,
        pltpu.roll(jnp.where(lane < 32, far, near), 96, 1),
        pltpu.roll(jnp.where(lane < 64, far, near), 64, 1),
    )


def product(high, low, kh_ref, kl_ref, z):
    kept = jnp.concatenate([h[48 * z : 48 * z + 192] for h in high], axis=0)
    rest = jnp.concatenate([h[48 * z : 48 * z + 192] for h in low], axis=0)
    both = dot(kh_ref[z], jnp.concatenate([kept, rest], axis=1))
    return own_lanes(both[:, 0:128] + both[:, 128:256] + dot(kl_ref[z], kept))


def gathered(own_ref, left_ref, right_ref):
    near = jnp.concatenate(
        [left_ref[:, 0:128], own_ref[0, :, 0:128], own_ref[1, :, 0:128], right_ref[0:96, 0:128]], axis=0
    )
    far = jnp.concatenate(
        [left_ref[:, 128:256], own_ref[0, :, 128:256], own_ref[1, :, 128:256], right_ref[0:96, 128:256]], axis=0
    )
    return views(near, far)


def sweep_kernel(top, own_ref, left_ref, right_ref, g_ref, ah_ref, al_ref, bh_ref, bl_ref, x_ref, rows, closed):
    seen = jnp.concatenate([left_ref[...], own_ref[0], own_ref[1], right_ref[0:96]], axis=0)
    look = [pltpu.roll(seen, 384 - 32 * start, 1)[:, 0:256] for start in (1, 2, 3, 4)]
    pairs = [split(view) for view in look]
    rows[24:32] = jnp.zeros((8, 256), F32)
    for z in range(2):
        kept = jnp.concatenate([p[0][48 * z : 48 * z + 192] for p in pairs], axis=0)
        rest = jnp.concatenate([p[1][48 * z : 48 * z + 192] for p in pairs], axis=0)
        both = dot(ah_ref[z], jnp.concatenate([kept, rest], axis=1))
        found = by_x(both[:, 0:256] + both[:, 256:512] + dot(al_ref[z], kept), 8, 24)
        rows[0:24] = g_ref[z] - found
        found = by_x(three(bh_ref[z, 48:240, 0:32], bl_ref[z, 48:240, 0:32], rows[...]), 8, 24)
        rows[0:24] = found
        at = 48 * z + 48
        body_rows = look[1][at : at + 16] + rows[0:16]
        body_rows = jnp.where(lax.broadcasted_iota(jnp.int32, (16, 256), 0) < 15, body_rows, 0.0)
        closed[...] = jnp.zeros((16, 256), F32)
        closed[6:15] = rows[15:24]
        after = look[2][at : at + 16] + closed[...]
        row = lax.broadcasted_iota(jnp.int32, (16, 256), 0)
        after = jnp.where((row >= 6) & (row < 15), after, 0.0)
        if top == 5:
            pad = jnp.zeros((16, 128), F32)
            body_rows = pltpu.roll(jnp.concatenate([body_rows, pad], axis=1), 64, 1)
            after = pltpu.roll(jnp.concatenate([after, pad], axis=1), 96, 1)
            x_ref[z] = jnp.where(lanes((16, 384)) // 32 == 10, after, body_rows)
        else:
            after = pltpu.roll(after, 32, 1)
            use = (lanes((16, 256)) // 32 == 7) & (row >= 6)
            x_ref[z] = pltpu.roll(jnp.where(use, after, body_rows), 192, 1)


def average_kernel(g_ref, right_ref, wide_ref, out_ref, ahead):
    for z in range(3):
        source = g_ref.at[z] if z < 2 else right_ref.at[96:112]
        ahead[z, 0:16] = source[:, 128:256]
        ahead[z, 16:32] = views(source[:, 128:256], source[:, 256:384])[2]
    for z in range(2):
        wide_ref[z] = jnp.zeros((48, 128), F32)
        for edge in range(12):
            ox, _, oz = OFFSETS[edge]
            start = 16 * ox + 3 * slot_of(edge)
            value = ahead[z + oz, start : start + 3]
            wide_ref[z, 3 * edge : 3 * edge + 3] = value
        write(out_ref, z, wide_ref[z, 0:36])


def write(out_ref, z, value):
    for x in range(4):
        out_ref[x, z] = value[:, 32 * x : 32 * x + 32]


def last_kernel(own_ref, left_ref, right_ref, wide_ref, ah_ref, al_ref, bh_ref, bl_ref, out_ref, rows, ahead, state):
    seen = gathered(own_ref, left_ref, right_ref)
    pairs = [split(view) for view in seen]
    high, low = [p[0] for p in pairs], [p[1] for p in pairs]
    for z in range(3):
        ahead[z, 0:16] = seen[1][48 * z + 48 : 48 * z + 64]
        ahead[z, 16:32] = seen[2][48 * z + 48 : 48 * z + 64]
    for z in range(2):
        for edge in range(12):
            ox, _, oz = OFFSETS[edge]
            start = 16 * ox + 3 * slot_of(edge)
            state[3 * edge : 3 * edge + 3] = ahead[z + oz, start : start + 3]
        rows[...] = jnp.zeros((48, 128), F32)
        rows[0:36] = wide_ref[z, 0:36] - product(high, low, ah_ref, al_ref, z)[0:36]
        write(out_ref, z, state[0:36] + solve(bh_ref[z, :, 0:48], bl_ref[z, :, 0:48], rows)[0:36])


def body(displacement, dof_weight, coarse_matrix, block_inverse):
    weights = jnp.transpose(dof_weight[:, 0], (2, 1, 0, 3))
    sums = call(numer_kernel, shape(2, 48, 128), flops=20_000_000)(displacement[:, 0], weights)
    left, right = shifted(sums, "gx", 1), shifted(sums, "gx", -1)
    matrix = jnp.transpose(coarse_matrix[:, 0], (0, 2, 3, 1, 4)).reshape(4, 27, 72, 36)
    block = jnp.transpose(block_inverse[:, 0], (0, 2, 1, 3)).reshape(4, 72, 36)
    ah, al, bh, bl, sent = prepare(matrix, block)
    left, right, sent = lax.optimization_barrier((left, right, sent))
    sums, up = call(sum_x_kernel, (shape(2, 32, 384), shape(24, 384)))(sums, left, right)
    left = shifted(up, "gz", 1)
    rows_left, rows_right = shifted(sent[2:4], "gx", 1), shifted(sent[0:2], "gx", -1)
    lower, upper, middle = call(sum_z_kernel, (shape(2, 8, 384),) * 3)(sums, left)
    below, above = shifted(upper, "gy", 1), shifted(lower, "gy", -1)
    wide = (shape(2, 192, 768, dtype=BF16),) * 2 + (shape(2, 288, 128, dtype=BF16),) * 2
    operator = call(merge_kernel, wide, flops=10_000_000)(sent, rows_left, rows_right)
    g, near, x = call(
        first_kernel,
        (shape(2, 16, 384), shape(2, 24, 256), shape(2, 16, 384)),
        (pltpu.VMEM((32, 384), F32),),
    )(lower, upper, middle, below, above, operator[2], operator[3])
    for sweep in range(3):
        below, above = shifted(x, "gy", 1), shifted(x, "gy", -1)
        own = jnp.concatenate([x, below, above], axis=1)
        left = shifted(own[1], "gz", 1)
        moving = own.reshape(96, own.shape[2])
        if sweep == 0:
            moving = jnp.concatenate([moving, g[0]], axis=0)
        right = shifted(moving, "gz", -1)
        if sweep == 0:
            every, average = call(
                average_kernel, (shape(2, 48, 128), shape(4, 2, 36, 32)), (pltpu.VMEM((3, 32, 128), F32),)
            )(g, right)
        if sweep < 2:
            x = call(
                functools.partial(sweep_kernel, 5 - sweep),
                shape(2, 16, 384 if sweep == 0 else 256),
                (pltpu.VMEM((32, 256), F32), pltpu.VMEM((16, 256), F32)),
                flops=20_000_000,
            )(own, left, right, near, *operator)
    x = call(
        last_kernel,
        shape(4, 2, 36, 32),
        (pltpu.VMEM((48, 128), F32), pltpu.VMEM((3, 32, 128), F32), pltpu.VMEM((40, 128), F32)),
        flops=10_000_000,
    )(own, left, right, every, ah, al, bh, bl)
    return average.reshape(4, 1, 2, 12, 3, 32), x.reshape(4, 1, 2, 36, 32)


def solution(mesh):
    placed = (
        P("gx", "gy", "gz", None, None, None, None),
        P("gx", "gy", "gz", None, None),
        P("gx", "gy", "gz", None, None, None),
        P("gx", "gy", "gz", None, None),
    )
    return jax.shard_map(
        body,
        mesh=mesh,
        in_specs=placed,
        out_specs=(P("gx", "gy", "gz", None, None, None), P("gx", "gy", "gz", None, None)),
        check_vma=False,
    )
```

```python
import functools

import jax
import jax.numpy as jnp
import numpy as np
from jax import lax
from jax.experimental import pallas as pl
from jax.experimental.pallas import tpu as pltpu
from jax.sharding import PartitionSpec as P


F32 = jnp.float32
BF16 = jnp.bfloat16
OFFSETS = (
    (0, 0, 0), (0, 0, 1), (0, 1, 0), (0, 1, 1),
    (0, 0, 0), (0, 0, 1), (1, 0, 0), (1, 0, 1),
    (0, 0, 0), (0, 1, 0), (1, 0, 0), (1, 1, 0),
)
WIDE_EDGES = (0, 2, 4, 8, 9, 6, 10, 11)


def slot_of(edge):
    direction = edge // 4
    upper = OFFSETS[edge][1]
    return (0 + upper, 2, 3 + upper)[direction]


def placement():
    table = np.zeros((1024, 768), np.float32)
    for offset in range(27):
        dx, dy, dz = offset // 9 - 1, offset // 3 % 3 - 1, offset % 3 - 1
        for edge in range(12):
            ox, oy, oz = OFFSETS[edge]
            direction = edge // 4
            if direction == 1:
                group, slot = {-1: (1, 2), 0: (0, 2), 1: (2, 2)}[dy + oy]
            else:
                base = 0 if direction == 0 else 3
                group, slot = {-1: (1, base), 0: (0, base), 1: (0, base + 1), 2: (2, base + 1)}[dy + oy]
            for comp in range(3):
                row = 16 * group + 3 * slot + comp
                table[36 * offset + 3 * edge + comp, 192 * (dx + ox + 1) + 48 * (dz + oz + 1) + row] = 1.0
    return table


def choice():
    table = np.zeros((512, 128), np.float32)
    for x in range(4):
        for place, edge in enumerate(WIDE_EDGES):
            for comp in range(3):
                table[128 * x + 3 * edge + comp, 32 * x + 3 * place + comp] = 1.0
    return table


def shifted(block, axis, distance):
    count = lax.axis_size(axis)
    return lax.ppermute(block, axis, [((i - distance) % count, i) for i in range(count)])


def lanes(shape):
    return lax.broadcasted_iota(jnp.int32, shape, len(shape) - 1)


def split(value):
    high = value.astype(BF16)
    return high, (value - high.astype(F32)).astype(BF16)


def dot(a, b):
    return jnp.dot(a, b, preferred_element_type=F32)


def own_lanes(value):
    group = lanes((40, 128)) // 32
    total = jnp.where(group == 0, value[0:40], 0.0)
    for x in range(1, 4):
        total = total + jnp.where(group == x, value[40 * x : 40 * x + 40], 0.0)
    return total


def call(kernel, outs, scratch=(), flops=1_000_000, **options):
    return pl.pallas_call(
        kernel,
        out_shape=outs,
        scratch_shapes=list(scratch),
        cost_estimate=pl.CostEstimate(flops=flops, bytes_accessed=1_000_000, transcendentals=0),
        compiler_params=pltpu.CompilerParams(vmem_limit_bytes=40 * 1024 * 1024),
        **options,
    )


def shape(*dims, dtype=F32):
    return jax.ShapeDtypeStruct(dims, dtype)


def numer_kernel(disp_ref, weight_ref, block_ref, choice_ref, sums_ref, weights, packed, rows):
    step = pl.program_id(0)

    @pl.when(step == 0)
    def _():
        weights[...] = weight_ref[...].astype(F32)
        packed[...] = jnp.zeros((4, 72, 128), F32)
        for x in range(4):
            packed[x, :, 0:36] = block_ref[x]
        for z in range(2):
            value = jnp.concatenate([packed[x, pl.ds(z, 36, stride=2), :] for x in range(4)], axis=1)
            high, low = split(value)
            rows[0:36] = dot(high, choice_ref[...]) + dot(low, choice_ref[...])
            for place, edge in enumerate(WIDE_EDGES):
                sums_ref[z, 48 + 3 * place : 51 + 3 * place] = rows[3 * edge : 3 * edge + 3]

    ones = jnp.ones((128, 128), BF16)
    group = (lanes((4, 512)) % 128) // 32
    keep = group == lax.broadcasted_iota(jnp.int32, (4, 512), 0)
    for z in range(2):
        pieces = []
        for edge in range(2):
            parts = [disp_ref[x, z, edge, c] for c in range(3) for x in range(4)]
            right = jnp.concatenate(parts + [ones], axis=0)
            at = 4 * step + 2 * edge + z
            left = jnp.concatenate([weights[x, pl.ds(at, 1), :] for x in range(4)], axis=0).astype(BF16)
            found = lax.dot_general(left, right, (((1,), (1,)), ((), ())), preferred_element_type=F32)
            row = jnp.sum(jnp.where(keep, found, 0.0), axis=0, keepdims=True)
            pieces = pieces + [row[:, 128 * c : 128 * c + 128] for c in range(4)]
        sums_ref[z, pl.ds(pl.multiple_of(8 * step, 8), 8), :] = jnp.concatenate(pieces, axis=0)


def sum_x_kernel(sums_ref, left_ref, right_ref, out_ref, up_ref):
    for z in range(2):
        all_x = jnp.concatenate([left_ref[z, 0:48], sums_ref[z, 0:48], right_ref[z, 0:48]], axis=1)
        below = pltpu.roll(all_x, 32, 1)
        out_ref[z, 0:16] = all_x[0:16]
        out_ref[z, 16:24] = all_x[16:24] + below[24:32]
        out_ref[z, 24:32] = all_x[32:40] + below[40:48]
    up_ref[...] = out_ref[1, 0:24]


def sum_z_kernel(sums_ref, left_ref, lower_ref, upper_ref, middle_ref):
    for z in range(2):
        below = left_ref if z == 0 else sums_ref.at[0]
        lower_ref[z, 0:4] = sums_ref[z, 0:4] + below[4:8]
        lower_ref[z, 4:8] = sums_ref[z, 24:28]
        upper_ref[z, 0:4] = sums_ref[z, 8:12] + below[12:16]
        upper_ref[z, 4:8] = sums_ref[z, 28:32]
        middle_ref[z, 0:4] = sums_ref[z, 16:20] + below[20:24]
        middle_ref[z, 4:8] = sums_ref[z, 16:20]


def by_x(value, count, rows):
    group = lanes((rows, value.shape[1])) // 32
    total = jnp.where(group == 0, value[0:rows], 0.0)
    for x in range(1, count):
        total = total + jnp.where(group == x, value[rows * x : rows * x + rows], 0.0)
    return total


def three(high, low, value):
    kept, rest = split(value)
    return dot(high, kept) + dot(high, rest) + dot(low, kept)


def solve(block_high, block_low, rows_ref):
    return own_lanes(three(block_high, block_low, rows_ref[...]))


def first_kernel(
    lower_ref, upper_ref, middle_ref, below_ref, above_ref, own_ref, left_ref, right_ref,
    g_ref, wide_ref, x_ref, bh_ref, bl_ref, rows,
):
    for z in range(2):
        rows[...] = jnp.zeros((32, 384), F32)
        node = lower_ref[z] + below_ref[z]
        top = upper_ref[z] + above_ref[z]
        middle = middle_ref[z]
        for slot, (source, at) in enumerate(((node, 0), (top, 0), (middle, 0), (node, 4), (top, 4))):
            rows[3 * slot : 3 * slot + 3] = source[at : at + 3] / source[at + 3 : at + 4]
        parts = [ref[z, 48:72, 32 * x : 32 * x + 32] for ref in (left_ref, own_ref, right_ref) for x in range(4)]
        high, low = split(jnp.concatenate(parts, axis=0))
        bh_ref[z], bl_ref[z] = high[48:240], low[48:240]
        found = by_x(three(high, low, rows[...]), 12, 24)
        x_ref[z] = jnp.where(lax.broadcasted_iota(jnp.int32, (16, 384), 0) < 15, found[0:16], 0.0)
        g_ref[z] = rows[0:16]
        wide_ref[z, 0:16] = pltpu.roll(rows[0:16], 320, 1)[:, 0:256]
        wide_ref[z, 15:24] = pltpu.roll(rows[0:16], 288, 1)[6:15, 0:256]


def pick(rows_ref, value):
    rows_ref[...] = value
    return [rows_ref[3 * edge : 3 * edge + 3] for edge in WIDE_EDGES]


def prepare_kernel(
    matrix_ref, block_ref, place_ref, ah_ref, al_ref, bh_ref, bl_ref, out_ref, packed, stacked, full
):
    packed[7] = jnp.zeros((72, 128), F32)
    for offset in range(27):
        start, tile = 36 * offset % 128, 36 * offset // 128
        size = min(36, 128 - start)
        packed[tile, :, start : start + size] = matrix_ref[0, offset, :, 0:size]
        if size < 36:
            packed[tile + 1, :, 0 : 36 - size] = matrix_ref[0, offset, :, size:36]
    for z in range(2):
        high, low = split(jnp.concatenate([packed[k, pl.ds(z, 36, stride=2), :] for k in range(8)], axis=1))
        pad = jnp.zeros((4, 1024), BF16)
        stacked[40 * z : 40 * z + 40] = jnp.concatenate([high, pad], axis=0)
        stacked[80 + 40 * z : 120 + 40 * z] = jnp.concatenate([low, pad], axis=0)
    found = dot(stacked[...], place_ref[...])
    for z in range(2):
        high, low = found[40 * z : 40 * z + 40], found[80 + 40 * z : 120 + 40 * z]
        ah_ref[z, 0] = high.astype(BF16)
        al_ref[z, 0] = low.astype(BF16)
        for place, value in enumerate(pick(full, high + low)):
            out_ref[0, z, 3 * place : 3 * place + 3] = value
    packed[0] = jnp.zeros((72, 128), F32)
    packed[0, :, 0:36] = block_ref[0]
    for z in range(2):
        high, low = split(packed[0, pl.ds(z, 36, stride=2), :])
        pad = jnp.zeros((4, 128), BF16)
        bh_ref[z, 0] = jnp.concatenate([high, pad], axis=0)
        bl_ref[z, 0] = jnp.concatenate([low, pad], axis=0)


def prepare(matrix, block):
    outs = (shape(2, 4, 40, 768, dtype=BF16),) * 2 + (shape(2, 4, 40, 128, dtype=BF16),) * 2
    outs = outs + (shape(4, 2, 24, 768),)
    wide = pl.BlockSpec((2, 1, 40, 768), lambda i: (0, i, 0, 0))
    slim = pl.BlockSpec((2, 1, 40, 128), lambda i: (0, i, 0, 0))
    ah, al, bh, bl, sent = call(
        prepare_kernel,
        outs,
        (
            pltpu.VMEM((8, 72, 128), F32),
            pltpu.VMEM((160, 1024), BF16),
            pltpu.VMEM((40, 768), F32),
        ),
        flops=20_000_000,
        grid=(4,),
        in_specs=[
            pl.BlockSpec((1, 27, 72, 36), lambda i: (i, 0, 0, 0)),
            pl.BlockSpec((1, 72, 36), lambda i: (i, 0, 0)),
            pl.BlockSpec((1024, 768), lambda i: (0, 0)),
        ],
        out_specs=(wide, wide, slim, slim, pl.BlockSpec((1, 2, 24, 768), lambda i: (i, 0, 0, 0))),
    )(matrix, block, jnp.asarray(placement(), BF16))
    return (
        ah.reshape(2, 160, 768), al.reshape(2, 160, 768),
        bh.reshape(2, 160, 128), bl.reshape(2, 160, 128), sent,
    )


def merge_kernel(own_ref, left_ref, right_ref, ah_ref, al_ref):
    for z in range(2):
        cells = [left_ref[0, z], left_ref[1, z]] + [own_ref[x, z] for x in range(4)]
        cells = cells + [right_ref[0, z], right_ref[1, z]]
        ah_ref[z], al_ref[z] = split(jnp.concatenate(cells, axis=0))


def views(near, far):
    lane = lanes(near.shape)
    return (
        pltpu.roll(jnp.where(lane >= 96, far, near), 32, 1),
        near,
        pltpu.roll(jnp.where(lane < 32, far, near), 96, 1),
        pltpu.roll(jnp.where(lane < 64, far, near), 64, 1),
    )


def product(high, low, kh_ref, kl_ref, z):
    kept = jnp.concatenate([h[48 * z : 48 * z + 192] for h in high], axis=0)
    rest = jnp.concatenate([h[48 * z : 48 * z + 192] for h in low], axis=0)
    both = dot(kh_ref[z], jnp.concatenate([kept, rest], axis=1))
    return own_lanes(both[:, 0:128] + both[:, 128:256] + dot(kl_ref[z], kept))


def gathered(own_ref, left_ref, right_ref):
    near = jnp.concatenate(
        [left_ref[:, 0:128], own_ref[0, :, 0:128], own_ref[1, :, 0:128], right_ref[0:96, 0:128]], axis=0
    )
    far = jnp.concatenate(
        [left_ref[:, 128:256], own_ref[0, :, 128:256], own_ref[1, :, 128:256], right_ref[0:96, 128:256]], axis=0
    )
    return views(near, far)


def sweep_kernel(top, own_ref, left_ref, right_ref, g_ref, ah_ref, al_ref, bh_ref, bl_ref, x_ref, rows, closed):
    seen = jnp.concatenate([left_ref[...], own_ref[0], own_ref[1], right_ref[0:96]], axis=0)
    look = [pltpu.roll(seen, 384 - 32 * start, 1)[:, 0:256] for start in (1, 2, 3, 4)]
    pairs = [split(view) for view in look]
    rows[24:32] = jnp.zeros((8, 256), F32)
    for z in range(2):
        kept = jnp.concatenate([p[0][48 * z : 48 * z + 192] for p in pairs], axis=0)
        rest = jnp.concatenate([p[1][48 * z : 48 * z + 192] for p in pairs], axis=0)
        both = dot(ah_ref[z], jnp.concatenate([kept, rest], axis=1))
        found = by_x(both[:, 0:256] + both[:, 256:512] + dot(al_ref[z], kept), 8, 24)
        rows[0:24] = g_ref[z] - found
        found = by_x(three(bh_ref[z], bl_ref[z], rows[...]), 8, 24)
        rows[0:24] = found
        at = 48 * z + 48
        body_rows = look[1][at : at + 16] + rows[0:16]
        body_rows = jnp.where(lax.broadcasted_iota(jnp.int32, (16, 256), 0) < 15, body_rows, 0.0)
        closed[...] = jnp.zeros((16, 256), F32)
        closed[6:15] = rows[15:24]
        after = look[2][at : at + 16] + closed[...]
        row = lax.broadcasted_iota(jnp.int32, (16, 256), 0)
        after = jnp.where((row >= 6) & (row < 15), after, 0.0)
        if top == 5:
            pad = jnp.zeros((16, 128), F32)
            body_rows = pltpu.roll(jnp.concatenate([body_rows, pad], axis=1), 64, 1)
            after = pltpu.roll(jnp.concatenate([after, pad], axis=1), 96, 1)
            x_ref[z] = jnp.where(lanes((16, 384)) // 32 == 10, after, body_rows)
        else:
            after = pltpu.roll(after, 32, 1)
            use = (lanes((16, 256)) // 32 == 7) & (row >= 6)
            x_ref[z] = pltpu.roll(jnp.where(use, after, body_rows), 192, 1)


def average_kernel(g_ref, right_ref, wide_ref, out_ref, ahead):
    for z in range(3):
        source = g_ref.at[z] if z < 2 else right_ref.at[96:112]
        ahead[z, 0:16] = source[:, 128:256]
        ahead[z, 16:32] = views(source[:, 128:256], source[:, 256:384])[2]
    for z in range(2):
        wide_ref[z] = jnp.zeros((48, 128), F32)
        for edge in range(12):
            ox, _, oz = OFFSETS[edge]
            start = 16 * ox + 3 * slot_of(edge)
            value = ahead[z + oz, start : start + 3]
            wide_ref[z, 3 * edge : 3 * edge + 3] = value
        write(out_ref, z, wide_ref[z, 0:36])


def write(out_ref, z, value):
    for x in range(4):
        out_ref[x, z] = value[:, 32 * x : 32 * x + 32]


def last_kernel(own_ref, left_ref, right_ref, wide_ref, ah_ref, al_ref, bh_ref, bl_ref, out_ref, rows, ahead, state):
    seen = gathered(own_ref, left_ref, right_ref)
    pairs = [split(view) for view in seen]
    high, low = [p[0] for p in pairs], [p[1] for p in pairs]
    state[...] = jnp.zeros((40, 128), F32)
    for z in range(3):
        ahead[z, 0:16] = seen[1][48 * z + 48 : 48 * z + 64]
        ahead[z, 16:32] = seen[2][48 * z + 48 : 48 * z + 64]
    for z in range(2):
        for edge in range(12):
            ox, _, oz = OFFSETS[edge]
            start = 16 * ox + 3 * slot_of(edge)
            state[3 * edge : 3 * edge + 3] = ahead[z + oz, start : start + 3]
        rows[...] = jnp.zeros((48, 128), F32)
        rows[0:36] = wide_ref[z, 0:36] - product(high, low, ah_ref, al_ref, z)[0:36]
        state[...] = state[...] + solve(bh_ref[z, :, 0:48], bl_ref[z, :, 0:48], rows)
        turned = state[...].T
        for x in range(4):
            out_ref[x, z] = turned[32 * x : 32 * x + 32, 0:36]


def after(value, *others):
    return lax.optimization_barrier((value, *others))[0]


def steps(displacement, dof_weight, coarse_matrix, block_inverse):
    weights = jnp.transpose(dof_weight[:, 0], (0, 2, 1, 3)).reshape(4, 24, 128)
    matrix = jnp.transpose(coarse_matrix[:, 0], (0, 2, 3, 1, 4)).reshape(4, 27, 72, 36)
    block = jnp.transpose(block_inverse[:, 0], (0, 2, 1, 3)).reshape(4, 72, 36)
    inputs = (displacement[:, 0], weights, block, jnp.asarray(choice(), BF16))
    sums = call(
        numer_kernel,
        shape(2, 72, 128),
        (pltpu.VMEM((4, 24, 128), F32), pltpu.VMEM((4, 72, 128), F32), pltpu.VMEM((40, 128), F32)),
        flops=20_000_000,
        grid=(6,),
        in_specs=[
            pl.BlockSpec((4, 2, 2, 3, 32, 128), lambda i: (0, 0, i, 0, 0, 0)),
            pl.BlockSpec((4, 24, 128), lambda i: (0, 0, 0)),
            pl.BlockSpec((4, 72, 36), lambda i: (0, 0, 0)),
            pl.BlockSpec((512, 128), lambda i: (0, 0)),
        ],
        out_specs=pl.BlockSpec((2, 72, 128), lambda i: (0, 0, 0)),
    )(*(pltpu.with_memory_space_constraint(a, pltpu.HBM) for a in inputs))
    mine, left, right = sums, shifted(sums, "gx", 1), shifted(sums, "gx", -1)
    sides = (mine, left, right)
    sums, up = call(sum_x_kernel, (shape(2, 32, 384), shape(24, 384)))(*sides)
    left = shifted(up, "gz", 1)
    ah, al, bh, bl, sent = prepare(after(matrix, up), block)
    lower, upper, middle = call(sum_z_kernel, (shape(2, 8, 384),) * 3)(sums, left)
    below, above = shifted(upper, "gy", 1), shifted(lower, "gy", -1)
    g, near, x, near_high, near_low = call(
        first_kernel,
        (shape(2, 16, 384), shape(2, 24, 256), shape(2, 16, 384)) + (shape(2, 192, 32, dtype=BF16),) * 2,
        (pltpu.VMEM((32, 384), F32),),
    )(lower, upper, middle, below, above, *sides)
    sent = after(sent, x)
    rows_left = shifted(sent[2:4], "gx", 1)
    rows_right = shifted(sent[0:2], "gx", -1)
    for sweep in range(3):
        below = shifted(x, "gy", 1)
        above = shifted(x, "gy", -1)
        if sweep == 0:
            rows_left = after(rows_left, below, above)
            wide = (shape(2, 192, 768, dtype=BF16),) * 2
            operator = call(merge_kernel, wide, flops=10_000_000)(sent, rows_left, rows_right)
        own = jnp.concatenate([x, below, above], axis=1)
        left = shifted(own[1], "gz", 1)
        moving = own.reshape(96, own.shape[2])
        if sweep == 0:
            moving = jnp.concatenate([moving, g[0]], axis=0)
        right = shifted(moving, "gz", -1)
        if sweep == 0:
            every, average = call(
                average_kernel, (shape(2, 48, 128), shape(4, 2, 36, 32)), (pltpu.VMEM((3, 32, 128), F32),)
            )(g, right)
        if sweep < 2:
            x = call(
                functools.partial(sweep_kernel, 5 - sweep),
                shape(2, 16, 384 if sweep == 0 else 256),
                (pltpu.VMEM((32, 256), F32), pltpu.VMEM((16, 256), F32)),
                flops=20_000_000,
            )(own, left, right, near, *operator, near_high, near_low)
    x = call(
        last_kernel,
        shape(4, 2, 32, 36),
        (pltpu.VMEM((48, 128), F32), pltpu.VMEM((3, 32, 128), F32), pltpu.VMEM((40, 128), F32)),
        flops=10_000_000,
    )(own, left, right, every, ah, al, bh, bl)
    return average.reshape(4, 1, 2, 12, 3, 32), jnp.swapaxes(x, 2, 3)[:, None]


def solution(mesh):
    placed = (
        P("gx", "gy", "gz", None, None, None, None),
        P("gx", "gy", "gz", None, None),
        P("gx", "gy", "gz", None, None, None),
        P("gx", "gy", "gz", None, None),
    )
    return jax.shard_map(
        steps,
        mesh=mesh,
        in_specs=placed,
        out_specs=(P("gx", "gy", "gz", None, None, None), P("gx", "gy", "gz", None, None)),
        check_vma=False,
    )
```

```python
import functools

import jax
import jax.numpy as jnp
import numpy as np
from jax import lax
from jax.experimental import pallas as pl
from jax.experimental.pallas import tpu as pltpu
from jax.sharding import PartitionSpec as P


F32 = jnp.float32
BF16 = jnp.bfloat16
OFFSETS = (
    (0, 0, 0), (0, 0, 1), (0, 1, 0), (0, 1, 1),
    (0, 0, 0), (0, 0, 1), (1, 0, 0), (1, 0, 1),
    (0, 0, 0), (0, 1, 0), (1, 0, 0), (1, 1, 0),
)
WIDE_EDGES = (0, 2, 4, 8, 9, 6, 10, 11)


def slot_of(edge):
    direction = edge // 4
    upper = OFFSETS[edge][1]
    return (0 + upper, 2, 3 + upper)[direction]


def placement():
    table = np.zeros((1024, 768), np.float32)
    for offset in range(27):
        dx, dy, dz = offset // 9 - 1, offset // 3 % 3 - 1, offset % 3 - 1
        for edge in range(12):
            ox, oy, oz = OFFSETS[edge]
            direction = edge // 4
            if direction == 1:
                group, slot = {-1: (1, 2), 0: (0, 2), 1: (2, 2)}[dy + oy]
            else:
                base = 0 if direction == 0 else 3
                group, slot = {-1: (1, base), 0: (0, base), 1: (0, base + 1), 2: (2, base + 1)}[dy + oy]
            for comp in range(3):
                row = 16 * group + 3 * slot + comp
                table[36 * offset + 3 * edge + comp, 192 * (dx + ox + 1) + 48 * (dz + oz + 1) + row] = 1.0
    return table


def choice():
    table = np.zeros((512, 128), np.float32)
    for x in range(4):
        for place, edge in enumerate(WIDE_EDGES):
            for comp in range(3):
                table[128 * x + 3 * edge + comp, 32 * x + 3 * place + comp] = 1.0
    return table


def shifted(block, axis, distance):
    count = lax.axis_size(axis)
    return lax.ppermute(block, axis, [((i - distance) % count, i) for i in range(count)])


def lanes(shape):
    return lax.broadcasted_iota(jnp.int32, shape, len(shape) - 1)


def split(value):
    high = value.astype(BF16)
    return high, (value - high.astype(F32)).astype(BF16)


def dot(a, b):
    return jnp.dot(a, b, preferred_element_type=F32)


def own_lanes(value):
    group = lanes((40, 128)) // 32
    total = jnp.where(group == 0, value[0:40], 0.0)
    for x in range(1, 4):
        total = total + jnp.where(group == x, value[40 * x : 40 * x + 40], 0.0)
    return total


def call(kernel, outs, scratch=(), flops=1_000_000, **options):
    return pl.pallas_call(
        kernel,
        out_shape=outs,
        scratch_shapes=list(scratch),
        cost_estimate=pl.CostEstimate(flops=flops, bytes_accessed=1_000_000, transcendentals=0),
        compiler_params=pltpu.CompilerParams(vmem_limit_bytes=40 * 1024 * 1024),
        **options,
    )


def streamed(*arrays):
    return [pltpu.with_memory_space_constraint(a, pltpu.HBM) for a in arrays]


def shape(*dims, dtype=F32):
    return jax.ShapeDtypeStruct(dims, dtype)


def numer_kernel(disp_ref, weight_ref, block_ref, choice_ref, sums_ref, weights, packed, rows):
    step = pl.program_id(0)

    @pl.when(step == 0)
    def _():
        weights[...] = weight_ref[...].astype(F32)
        packed[...] = jnp.zeros((4, 72, 128), F32)
        for x in range(4):
            packed[x, :, 0:36] = block_ref[x]
        for z in range(2):
            value = jnp.concatenate([packed[x, pl.ds(z, 36, stride=2), :] for x in range(4)], axis=1)
            high, low = split(value)
            rows[0:36] = dot(high, choice_ref[...]) + dot(low, choice_ref[...])
            for place, edge in enumerate(WIDE_EDGES):
                sums_ref[z, 48 + 3 * place : 51 + 3 * place] = rows[3 * edge : 3 * edge + 3]

    ones = jnp.ones((128, 128), BF16)
    group = (lanes((4, 512)) % 128) // 32
    keep = group == lax.broadcasted_iota(jnp.int32, (4, 512), 0)
    for z in range(2):
        pieces = []
        for edge in range(2):
            parts = [disp_ref[x, z, edge, c] for c in range(3) for x in range(4)]
            right = jnp.concatenate(parts + [ones], axis=0)
            at = 4 * step + 2 * edge + z
            left = jnp.concatenate([weights[x, pl.ds(at, 1), :] for x in range(4)], axis=0).astype(BF16)
            found = lax.dot_general(left, right, (((1,), (1,)), ((), ())), preferred_element_type=F32)
            row = jnp.sum(jnp.where(keep, found, 0.0), axis=0, keepdims=True)
            pieces = pieces + [row[:, 128 * c : 128 * c + 128] for c in range(4)]
        sums_ref[z, pl.ds(pl.multiple_of(8 * step, 8), 8), :] = jnp.concatenate(pieces, axis=0)


def sum_x_kernel(sums_ref, left_ref, right_ref, out_ref, up_ref):
    for z in range(2):
        all_x = jnp.concatenate([left_ref[z, 0:48], sums_ref[z, 0:48], right_ref[z, 0:48]], axis=1)
        below = pltpu.roll(all_x, 32, 1)
        out_ref[z, 0:16] = all_x[0:16]
        out_ref[z, 16:24] = all_x[16:24] + below[24:32]
        out_ref[z, 24:32] = all_x[32:40] + below[40:48]
    up_ref[...] = out_ref[1, 0:24]


def sum_z_kernel(sums_ref, left_ref, lower_ref, upper_ref, middle_ref):
    for z in range(2):
        below = left_ref if z == 0 else sums_ref.at[0]
        lower_ref[z, 0:4] = sums_ref[z, 0:4] + below[4:8]
        lower_ref[z, 4:8] = sums_ref[z, 24:28]
        upper_ref[z, 0:4] = sums_ref[z, 8:12] + below[12:16]
        upper_ref[z, 4:8] = sums_ref[z, 28:32]
        middle_ref[z, 0:4] = sums_ref[z, 16:20] + below[20:24]
        middle_ref[z, 4:8] = sums_ref[z, 16:20]


def by_x(value, count, rows):
    group = lanes((rows, value.shape[1])) // 32
    total = jnp.where(group == 0, value[0:rows], 0.0)
    for x in range(1, count):
        total = total + jnp.where(group == x, value[rows * x : rows * x + rows], 0.0)
    return total


def three(high, low, value):
    kept, rest = split(value)
    return dot(high, kept) + dot(high, rest) + dot(low, kept)


def solve(block_high, block_low, rows_ref):
    return own_lanes(three(block_high, block_low, rows_ref[...]))


def first_kernel(
    lower_ref, upper_ref, middle_ref, below_ref, above_ref, own_ref, left_ref, right_ref,
    g_ref, wide_ref, x_ref, bh_ref, bl_ref, rows,
):
    for z in range(2):
        rows[...] = jnp.zeros((32, 384), F32)
        node = lower_ref[z] + below_ref[z]
        top = upper_ref[z] + above_ref[z]
        middle = middle_ref[z]
        for slot, (source, at) in enumerate(((node, 0), (top, 0), (middle, 0), (node, 4), (top, 4))):
            rows[3 * slot : 3 * slot + 3] = source[at : at + 3] / source[at + 3 : at + 4]
        parts = [ref[z, 48:72, 32 * x : 32 * x + 32] for ref in (left_ref, own_ref, right_ref) for x in range(4)]
        high, low = split(jnp.concatenate(parts, axis=0))
        bh_ref[z], bl_ref[z] = high[48:240], low[48:240]
        found = by_x(three(high, low, rows[...]), 12, 24)
        x_ref[z] = jnp.where(lax.broadcasted_iota(jnp.int32, (16, 384), 0) < 15, found[0:16], 0.0)
        g_ref[z] = rows[0:16]
        wide_ref[z, 0:16] = pltpu.roll(rows[0:16], 320, 1)[:, 0:256]
        wide_ref[z, 15:24] = pltpu.roll(rows[0:16], 288, 1)[6:15, 0:256]


def pick(rows_ref, value):
    rows_ref[...] = value
    return [rows_ref[3 * edge : 3 * edge + 3] for edge in WIDE_EDGES]


def prepare_kernel(
    matrix_ref, block_ref, place_ref, ah_ref, al_ref, bh_ref, bl_ref, out_ref, packed, stacked, full
):
    packed[7] = jnp.zeros((72, 128), F32)
    for offset in range(27):
        start, tile = 36 * offset % 128, 36 * offset // 128
        size = min(36, 128 - start)
        packed[tile, :, start : start + size] = matrix_ref[0, offset, :, 0:size]
        if size < 36:
            packed[tile + 1, :, 0 : 36 - size] = matrix_ref[0, offset, :, size:36]
    for z in range(2):
        high, low = split(jnp.concatenate([packed[k, pl.ds(z, 36, stride=2), :] for k in range(8)], axis=1))
        pad = jnp.zeros((4, 1024), BF16)
        stacked[40 * z : 40 * z + 40] = jnp.concatenate([high, pad], axis=0)
        stacked[80 + 40 * z : 120 + 40 * z] = jnp.concatenate([low, pad], axis=0)
    found = dot(stacked[...], place_ref[...])
    for z in range(2):
        high, low = found[40 * z : 40 * z + 40], found[80 + 40 * z : 120 + 40 * z]
        ah_ref[z, 0] = high.astype(BF16)
        al_ref[z, 0] = low.astype(BF16)
        for place, value in enumerate(pick(full, high + low)):
            out_ref[0, z, 3 * place : 3 * place + 3] = value
    packed[0] = jnp.zeros((72, 128), F32)
    packed[0, :, 0:36] = block_ref[0]
    for z in range(2):
        high, low = split(packed[0, pl.ds(z, 36, stride=2), :])
        pad = jnp.zeros((4, 128), BF16)
        bh_ref[z, 0] = jnp.concatenate([high, pad], axis=0)
        bl_ref[z, 0] = jnp.concatenate([low, pad], axis=0)


def prepare(matrix, block):
    outs = (shape(2, 4, 40, 768, dtype=BF16),) * 2 + (shape(2, 4, 40, 128, dtype=BF16),) * 2
    outs = outs + (shape(4, 2, 24, 768),)
    wide = pl.BlockSpec((2, 1, 40, 768), lambda i: (0, i, 0, 0))
    slim = pl.BlockSpec((2, 1, 40, 128), lambda i: (0, i, 0, 0))
    ah, al, bh, bl, sent = call(
        prepare_kernel,
        outs,
        (
            pltpu.VMEM((8, 72, 128), F32),
            pltpu.VMEM((160, 1024), BF16),
            pltpu.VMEM((40, 768), F32),
        ),
        flops=20_000_000,
        grid=(4,),
        in_specs=[
            pl.BlockSpec((1, 27, 72, 36), lambda i: (i, 0, 0, 0)),
            pl.BlockSpec((1, 72, 36), lambda i: (i, 0, 0)),
            pl.BlockSpec((1024, 768), lambda i: (0, 0)),
        ],
        out_specs=(wide, wide, slim, slim, pl.BlockSpec((1, 2, 24, 768), lambda i: (i, 0, 0, 0))),
    )(*streamed(matrix, block, jnp.asarray(placement(), BF16)))
    return (
        ah.reshape(2, 160, 768), al.reshape(2, 160, 768),
        bh.reshape(2, 160, 128), bl.reshape(2, 160, 128), sent,
    )


def merge_kernel(own_ref, left_ref, right_ref, ah_ref, al_ref):
    for z in range(2):
        cells = [left_ref[0, z], left_ref[1, z]] + [own_ref[x, z] for x in range(4)]
        cells = cells + [right_ref[0, z], right_ref[1, z]]
        ah_ref[z], al_ref[z] = split(jnp.concatenate(cells, axis=0))


def views(near, far):
    lane = lanes(near.shape)
    return (
        pltpu.roll(jnp.where(lane >= 96, far, near), 32, 1),
        near,
        pltpu.roll(jnp.where(lane < 32, far, near), 96, 1),
        pltpu.roll(jnp.where(lane < 64, far, near), 64, 1),
    )


def product(high, low, kh_ref, kl_ref, z):
    kept = jnp.concatenate([h[48 * z : 48 * z + 192] for h in high], axis=0)
    rest = jnp.concatenate([h[48 * z : 48 * z + 192] for h in low], axis=0)
    both = dot(kh_ref[z], jnp.concatenate([kept, rest], axis=1))
    return own_lanes(both[:, 0:128] + both[:, 128:256] + dot(kl_ref[z], kept))


def gathered(own_ref, left_ref, right_ref):
    near = jnp.concatenate(
        [left_ref[:, 0:128], own_ref[0, :, 0:128], own_ref[1, :, 0:128], right_ref[0:96, 0:128]], axis=0
    )
    far = jnp.concatenate(
        [left_ref[:, 128:256], own_ref[0, :, 128:256], own_ref[1, :, 128:256], right_ref[0:96, 128:256]], axis=0
    )
    return views(near, far)


def sweep_kernel(top, own_ref, left_ref, right_ref, g_ref, ah_ref, al_ref, bh_ref, bl_ref, x_ref, rows, closed):
    seen = jnp.concatenate([left_ref[...], own_ref[0], own_ref[1], right_ref[0:96]], axis=0)
    look = [pltpu.roll(seen, 384 - 32 * start, 1)[:, 0:256] for start in (1, 2, 3, 4)]
    pairs = [split(view) for view in look]
    rows[24:32] = jnp.zeros((8, 256), F32)
    for z in range(2):
        kept = jnp.concatenate([p[0][48 * z : 48 * z + 192] for p in pairs], axis=0)
        rest = jnp.concatenate([p[1][48 * z : 48 * z + 192] for p in pairs], axis=0)
        both = dot(ah_ref[z], jnp.concatenate([kept, rest], axis=1))
        found = by_x(both[:, 0:256] + both[:, 256:512] + dot(al_ref[z], kept), 8, 24)
        rows[0:24] = g_ref[z] - found
        found = by_x(three(bh_ref[z], bl_ref[z], rows[...]), 8, 24)
        rows[0:24] = found
        at = 48 * z + 48
        body_rows = look[1][at : at + 16] + rows[0:16]
        body_rows = jnp.where(lax.broadcasted_iota(jnp.int32, (16, 256), 0) < 15, body_rows, 0.0)
        closed[...] = jnp.zeros((16, 256), F32)
        closed[6:15] = rows[15:24]
        after = look[2][at : at + 16] + closed[...]
        row = lax.broadcasted_iota(jnp.int32, (16, 256), 0)
        after = jnp.where((row >= 6) & (row < 15), after, 0.0)
        if top == 5:
            pad = jnp.zeros((16, 128), F32)
            body_rows = pltpu.roll(jnp.concatenate([body_rows, pad], axis=1), 64, 1)
            after = pltpu.roll(jnp.concatenate([after, pad], axis=1), 96, 1)
            x_ref[z] = jnp.where(lanes((16, 384)) // 32 == 10, after, body_rows)
        else:
            after = pltpu.roll(after, 32, 1)
            use = (lanes((16, 256)) // 32 == 7) & (row >= 6)
            x_ref[z] = pltpu.roll(jnp.where(use, after, body_rows), 192, 1)


def average_kernel(g_ref, right_ref, wide_ref, out_ref, ahead):
    for z in range(3):
        source = g_ref.at[z] if z < 2 else right_ref.at[96:112]
        ahead[z, 0:16] = source[:, 128:256]
        ahead[z, 16:32] = views(source[:, 128:256], source[:, 256:384])[2]
    for z in range(2):
        wide_ref[z] = jnp.zeros((48, 128), F32)
        for edge in range(12):
            ox, _, oz = OFFSETS[edge]
            start = 16 * ox + 3 * slot_of(edge)
            value = ahead[z + oz, start : start + 3]
            wide_ref[z, 3 * edge : 3 * edge + 3] = value
        write(out_ref, z, wide_ref[z, 0:36])


def write(out_ref, z, value):
    for x in range(4):
        out_ref[x, z] = value[:, 32 * x : 32 * x + 32]


def last_kernel(own_ref, left_ref, right_ref, wide_ref, ah_ref, al_ref, bh_ref, bl_ref, out_ref, rows, ahead, state):
    seen = gathered(own_ref, left_ref, right_ref)
    pairs = [split(view) for view in seen]
    high, low = [p[0] for p in pairs], [p[1] for p in pairs]
    state[...] = jnp.zeros((40, 128), F32)
    for z in range(3):
        ahead[z, 0:16] = seen[1][48 * z + 48 : 48 * z + 64]
        ahead[z, 16:32] = seen[2][48 * z + 48 : 48 * z + 64]
    for z in range(2):
        for edge in range(12):
            ox, _, oz = OFFSETS[edge]
            start = 16 * ox + 3 * slot_of(edge)
            state[3 * edge : 3 * edge + 3] = ahead[z + oz, start : start + 3]
        rows[...] = jnp.zeros((48, 128), F32)
        rows[0:36] = wide_ref[z, 0:36] - product(high, low, ah_ref, al_ref, z)[0:36]
        state[...] = state[...] + solve(bh_ref[z, :, 0:48], bl_ref[z, :, 0:48], rows)
        turned = state[...].T
        for x in range(4):
            out_ref[x, z] = turned[32 * x : 32 * x + 32, 0:36]


def after(value, *others):
    return lax.optimization_barrier((value, *others))[0]


def steps(displacement, dof_weight, coarse_matrix, block_inverse):
    weights = jnp.transpose(dof_weight[:, 0], (0, 2, 1, 3)).reshape(4, 24, 128)
    matrix = jnp.transpose(coarse_matrix[:, 0], (0, 2, 3, 1, 4)).reshape(4, 27, 72, 36)
    block = jnp.transpose(block_inverse[:, 0], (0, 2, 1, 3)).reshape(4, 72, 36)
    sums = call(
        numer_kernel,
        shape(2, 72, 128),
        (pltpu.VMEM((4, 24, 128), F32), pltpu.VMEM((4, 72, 128), F32), pltpu.VMEM((40, 128), F32)),
        flops=20_000_000,
        grid=(6,),
        in_specs=[
            pl.BlockSpec((4, 2, 2, 3, 32, 128), lambda i: (0, 0, i, 0, 0, 0)),
            pl.BlockSpec((4, 24, 128), lambda i: (0, 0, 0)),
            pl.BlockSpec((4, 72, 36), lambda i: (0, 0, 0)),
            pl.BlockSpec((512, 128), lambda i: (0, 0)),
        ],
        out_specs=pl.BlockSpec((2, 72, 128), lambda i: (0, 0, 0)),
    )(*streamed(displacement[:, 0], weights, block, jnp.asarray(choice(), BF16)))
    mine, left, right = sums, shifted(sums, "gx", 1), shifted(sums, "gx", -1)
    sides = (mine, left, right)
    sums, up = call(sum_x_kernel, (shape(2, 32, 384), shape(24, 384)))(*sides)
    left = shifted(up, "gz", 1)
    ah, al, bh, bl, sent = prepare(after(matrix, up), block)
    lower, upper, middle = call(sum_z_kernel, (shape(2, 8, 384),) * 3)(sums, left)
    below = shifted(upper, "gy", 1)
    above = shifted(lower, "gy", -1)
    g, near, x, near_high, near_low = call(
        first_kernel,
        (shape(2, 16, 384), shape(2, 24, 256), shape(2, 16, 384)) + (shape(2, 192, 32, dtype=BF16),) * 2,
        (pltpu.VMEM((32, 384), F32),),
    )(lower, upper, middle, below, above, *sides)
    sent = after(sent, x)
    rows_left = shifted(sent[2:4], "gx", 1)
    rows_right = shifted(sent[0:2], "gx", -1)
    for sweep in range(3):
        below = shifted(x, "gy", 1)
        above = shifted(x, "gy", -1)
        if sweep == 0:
            rows_left = after(rows_left, below, above)
            wide = (shape(2, 192, 768, dtype=BF16),) * 2
            operator = call(merge_kernel, wide, flops=10_000_000)(sent, rows_left, rows_right)
        own = jnp.concatenate([x, below, above], axis=1)
        left = shifted(own[1], "gz", 1)
        moving = own.reshape(96, own.shape[2])
        if sweep == 0:
            moving = jnp.concatenate([moving, g[0]], axis=0)
        right = shifted(moving, "gz", -1)
        if sweep == 0:
            every, average = call(
                average_kernel, (shape(2, 48, 128), shape(4, 2, 36, 32)), (pltpu.VMEM((3, 32, 128), F32),)
            )(g, right)
        if sweep < 2:
            x = call(
                functools.partial(sweep_kernel, 5 - sweep),
                shape(2, 16, 384 if sweep == 0 else 256),
                (pltpu.VMEM((32, 256), F32), pltpu.VMEM((16, 256), F32)),
                flops=20_000_000,
            )(own, left, right, near, *operator, near_high, near_low)
    x = call(
        last_kernel,
        shape(4, 2, 32, 36),
        (pltpu.VMEM((48, 128), F32), pltpu.VMEM((3, 32, 128), F32), pltpu.VMEM((40, 128), F32)),
        flops=10_000_000,
    )(own, left, right, every, ah, al, bh, bl)
    return average.reshape(4, 1, 2, 12, 3, 32), jnp.swapaxes(x, 2, 3)[:, None]


def solution(mesh):
    placed = (
        P("gx", "gy", "gz", None, None, None, None),
        P("gx", "gy", "gz", None, None),
        P("gx", "gy", "gz", None, None, None),
        P("gx", "gy", "gz", None, None),
    )
    return jax.shard_map(
        steps,
        mesh=mesh,
        in_specs=placed,
        out_specs=(P("gx", "gy", "gz", None, None, None), P("gx", "gy", "gz", None, None)),
        check_vma=False,
    )
```

```python
import functools

import jax
import jax.numpy as jnp
import numpy as np
from jax import lax
from jax.experimental import pallas as pl
from jax.experimental.pallas import tpu as pltpu
from jax.sharding import PartitionSpec as P


F32 = jnp.float32
BF16 = jnp.bfloat16
OFFSETS = (
    (0, 0, 0), (0, 0, 1), (0, 1, 0), (0, 1, 1),
    (0, 0, 0), (0, 0, 1), (1, 0, 0), (1, 0, 1),
    (0, 0, 0), (0, 1, 0), (1, 0, 0), (1, 1, 0),
)
WIDE_EDGES = (0, 2, 4, 8, 9, 6, 10, 11)


def slot_of(edge):
    direction = edge // 4
    upper = OFFSETS[edge][1]
    return (0 + upper, 2, 3 + upper)[direction]


def placement():
    table = np.zeros((384, 384), np.float32)
    for offset in range(9):
        dy, dz = offset // 3 - 1, offset % 3 - 1
        for edge in range(12):
            ox, oy, oz = OFFSETS[edge]
            direction = edge // 4
            if direction == 1:
                group, slot = {-1: (1, 2), 0: (0, 2), 1: (2, 2)}[dy + oy]
            else:
                base = 0 if direction == 0 else 3
                group, slot = {-1: (1, base), 0: (0, base), 1: (0, base + 1), 2: (2, base + 1)}[dy + oy]
            for comp in range(3):
                row = 16 * group + 3 * slot + comp
                table[36 * offset + 3 * edge + comp, 192 * ox + 48 * (dz + oz + 1) + row] = 1.0
    return table


def choice():
    table = np.zeros((512, 128), np.float32)
    for x in range(4):
        for place, edge in enumerate(WIDE_EDGES):
            for comp in range(3):
                table[128 * x + 3 * edge + comp, 32 * x + 3 * place + comp] = 1.0
    return table


def shifted(block, axis, distance):
    count = lax.axis_size(axis)
    return lax.ppermute(block, axis, [((i - distance) % count, i) for i in range(count)])


def lanes(shape):
    return lax.broadcasted_iota(jnp.int32, shape, len(shape) - 1)


def split(value):
    high = value.astype(BF16)
    return high, (value - high.astype(F32)).astype(BF16)


def dot(a, b):
    return jnp.dot(a, b, preferred_element_type=F32)


def own_lanes(value):
    group = lanes((40, 128)) // 32
    total = jnp.where(group == 0, value[0:40], 0.0)
    for x in range(1, 4):
        total = total + jnp.where(group == x, value[40 * x : 40 * x + 40], 0.0)
    return total


def call(kernel, outs, scratch=(), flops=1_000_000, **options):
    return pl.pallas_call(
        kernel,
        out_shape=outs,
        scratch_shapes=list(scratch),
        cost_estimate=pl.CostEstimate(flops=flops, bytes_accessed=1_000_000, transcendentals=0),
        compiler_params=pltpu.CompilerParams(vmem_limit_bytes=40 * 1024 * 1024),
        **options,
    )


def streamed(*arrays):
    return [pltpu.with_memory_space_constraint(a, pltpu.HBM) for a in arrays]


def shape(*dims, dtype=F32):
    return jax.ShapeDtypeStruct(dims, dtype)


def pick(rows_ref, value):
    rows_ref[...] = value
    return [rows_ref[3 * edge : 3 * edge + 3] for edge in WIDE_EDGES]


def take_sums(step, disp_ref, weights, held):
    ones = jnp.ones((128, 128), BF16)
    group = (lanes((4, 512)) % 128) // 32
    keep = group == lax.broadcasted_iota(jnp.int32, (4, 512), 0)
    for z in range(2):
        pieces = []
        for edge in range(3):
            parts = [disp_ref[x, z, edge, c] for c in range(3) for x in range(4)]
            right = jnp.concatenate(parts + [ones], axis=0)
            at = 6 * step + 2 * edge + z
            left = jnp.concatenate([weights[x, pl.ds(at, 1), :] for x in range(4)], axis=0).astype(BF16)
            found = lax.dot_general(left, right, (((1,), (1,)), ((), ())), preferred_element_type=F32)
            row = jnp.sum(jnp.where(keep, found, 0.0), axis=0, keepdims=True)
            pieces = pieces + [row[:, 128 * c : 128 * c + 128] for c in range(4)]
        held[step, z, 0:12] = jnp.concatenate(pieces, axis=0)


def take_operator(matrix_ref, place_ref, ah_ref, al_ref, sent_ref, packed, stacked, full):
    for offset in range(27):
        start, tile = 36 * (offset % 9) % 128, 3 * (offset // 9) + 36 * (offset % 9) // 128
        size = min(36, 128 - start)
        packed[tile, :, start : start + size] = matrix_ref[0, offset, :, 0:size]
        if size < 36:
            packed[tile + 1, :, 0 : 36 - size] = matrix_ref[0, offset, :, size:36]
    pad = jnp.zeros((4, 384), BF16)
    found = []
    for dx in range(3):
        for z in range(2):
            high, low = split(
                jnp.concatenate([packed[3 * dx + k, pl.ds(z, 36, stride=2), :] for k in range(3)], axis=1)
            )
            stacked[40 * z : 40 * z + 40] = jnp.concatenate([high, pad], axis=0)
            stacked[80 + 40 * z : 120 + 40 * z] = jnp.concatenate([low, pad], axis=0)
        found.append(dot(stacked[...], place_ref[...]))
    none = jnp.zeros((160, 384), F32)
    total = jnp.concatenate([found[0], found[2]], axis=1)
    total = total + pltpu.roll(jnp.concatenate([found[1], none], axis=1), 192, 1)
    for z in range(2):
        high, low = total[40 * z : 40 * z + 40], total[80 + 40 * z : 120 + 40 * z]
        ah_ref[z, 0] = high.astype(BF16)
        al_ref[z, 0] = low.astype(BF16)
        for place, value in enumerate(pick(full, high + low)):
            sent_ref[0, z, 3 * place : 3 * place + 3] = value


def start_kernel(
    disp_ref, weight_ref, block_ref, choice_ref, matrix_ref, place_ref,
    sums_ref, ah_ref, al_ref, bh_ref, bl_ref, sent_ref,
    weights, inner, rows, held, packed, stacked, full,
):
    step = pl.program_id(0)

    @pl.when(step == 0)
    def _():
        weights[...] = weight_ref[...].astype(F32)
        inner[...] = jnp.zeros((4, 72, 128), F32)
        for tile in range(9):
            packed[tile] = jnp.zeros((72, 128), F32)
        for x in range(4):
            inner[x, :, 0:36] = block_ref[x]
        for z in range(2):
            value = jnp.concatenate([inner[x, pl.ds(z, 36, stride=2), :] for x in range(4)], axis=1)
            high, low = split(value)
            rows[0:36] = dot(high, choice_ref[...]) + dot(low, choice_ref[...])
            for place, edge in enumerate(WIDE_EDGES):
                sums_ref[z, 48 + 3 * place : 51 + 3 * place] = rows[3 * edge : 3 * edge + 3]

    take_sums(step, disp_ref, weights, held)
    take_operator(matrix_ref, place_ref, ah_ref, al_ref, sent_ref, packed, stacked, full)
    for z in range(2):
        high, low = split(inner[step, pl.ds(z, 36, stride=2), :])
        pad = jnp.zeros((4, 128), BF16)
        bh_ref[z, 0] = jnp.concatenate([high, pad], axis=0)
        bl_ref[z, 0] = jnp.concatenate([low, pad], axis=0)

    @pl.when(step == 3)
    def _():
        for z in range(2):
            for part in range(4):
                sums_ref[z, 12 * part : 12 * part + 12] = held[part, z, 0:12]


def start(displacement, weights, block, matrix):
    outs = (shape(2, 72, 128),) + (shape(2, 4, 40, 768, dtype=BF16),) * 2
    outs = outs + (shape(2, 4, 40, 128, dtype=BF16),) * 2 + (shape(4, 2, 24, 768),)
    wide = pl.BlockSpec((2, 1, 40, 768), lambda i: (0, i, 0, 0))
    slim = pl.BlockSpec((2, 1, 40, 128), lambda i: (0, i, 0, 0))
    sums, ah, al, bh, bl, sent = call(
        start_kernel,
        outs,
        (
            pltpu.VMEM((4, 24, 128), F32),
            pltpu.VMEM((4, 72, 128), F32),
            pltpu.VMEM((40, 128), F32),
            pltpu.VMEM((4, 2, 16, 128), F32),
            pltpu.VMEM((9, 72, 128), F32),
            pltpu.VMEM((160, 384), BF16),
            pltpu.VMEM((40, 768), F32),
        ),
        flops=40_000_000,
        grid=(4,),
        in_specs=[
            pl.BlockSpec((4, 2, 3, 3, 32, 128), lambda i: (0, 0, i, 0, 0, 0)),
            pl.BlockSpec((4, 24, 128), lambda i: (0, 0, 0)),
            pl.BlockSpec((4, 72, 36), lambda i: (0, 0, 0)),
            pl.BlockSpec((512, 128), lambda i: (0, 0)),
            pl.BlockSpec((1, 27, 72, 36), lambda i: (i, 0, 0, 0)),
            pl.BlockSpec((384, 384), lambda i: (0, 0)),
        ],
        out_specs=(
            pl.BlockSpec((2, 72, 128), lambda i: (0, 0, 0)),
            wide,
            wide,
            slim,
            slim,
            pl.BlockSpec((1, 2, 24, 768), lambda i: (i, 0, 0, 0)),
        ),
    )(*streamed(displacement, weights, block, jnp.asarray(choice(), BF16), matrix, jnp.asarray(placement(), BF16)))
    return (
        sums, ah.reshape(2, 160, 768), al.reshape(2, 160, 768),
        bh.reshape(2, 160, 128), bl.reshape(2, 160, 128), sent,
    )


def sum_x_kernel(sums_ref, left_ref, right_ref, out_ref, up_ref):
    for z in range(2):
        all_x = jnp.concatenate([left_ref[z, 0:48], sums_ref[z, 0:48], right_ref[z, 0:48]], axis=1)
        below = pltpu.roll(all_x, 32, 1)
        out_ref[z, 0:16] = all_x[0:16]
        out_ref[z, 16:24] = all_x[16:24] + below[24:32]
        out_ref[z, 24:32] = all_x[32:40] + below[40:48]
    up_ref[...] = out_ref[1, 0:24]


def sum_z_kernel(sums_ref, left_ref, lower_ref, upper_ref, middle_ref):
    for z in range(2):
        below = left_ref if z == 0 else sums_ref.at[0]
        lower_ref[z, 0:4] = sums_ref[z, 0:4] + below[4:8]
        lower_ref[z, 4:8] = sums_ref[z, 24:28]
        upper_ref[z, 0:4] = sums_ref[z, 8:12] + below[12:16]
        upper_ref[z, 4:8] = sums_ref[z, 28:32]
        middle_ref[z, 0:4] = sums_ref[z, 16:20] + below[20:24]
        middle_ref[z, 4:8] = sums_ref[z, 16:20]


def by_x(value, count, rows):
    group = lanes((rows, value.shape[1])) // 32
    total = jnp.where(group == 0, value[0:rows], 0.0)
    for x in range(1, count):
        total = total + jnp.where(group == x, value[rows * x : rows * x + rows], 0.0)
    return total


def three(high, low, value):
    kept, rest = split(value)
    return dot(high, kept) + dot(high, rest) + dot(low, kept)


def solve(block_high, block_low, rows_ref):
    return own_lanes(three(block_high, block_low, rows_ref[...]))


def first_kernel(
    lower_ref, upper_ref, middle_ref, below_ref, above_ref, own_ref, left_ref, right_ref,
    g_ref, wide_ref, x_ref, bh_ref, bl_ref, rows,
):
    for z in range(2):
        rows[...] = jnp.zeros((32, 384), F32)
        node = lower_ref[z] + below_ref[z]
        top = upper_ref[z] + above_ref[z]
        middle = middle_ref[z]
        for slot, (source, at) in enumerate(((node, 0), (top, 0), (middle, 0), (node, 4), (top, 4))):
            rows[3 * slot : 3 * slot + 3] = source[at : at + 3] / source[at + 3 : at + 4]
        parts = [ref[z, 48:72, 32 * x : 32 * x + 32] for ref in (left_ref, own_ref, right_ref) for x in range(4)]
        high, low = split(jnp.concatenate(parts, axis=0))
        bh_ref[z], bl_ref[z] = high[48:240], low[48:240]
        found = by_x(three(high, low, rows[...]), 12, 24)
        x_ref[z] = jnp.where(lax.broadcasted_iota(jnp.int32, (16, 384), 0) < 15, found[0:16], 0.0)
        g_ref[z] = rows[0:16]
        wide_ref[z, 0:16] = pltpu.roll(rows[0:16], 320, 1)[:, 0:256]
        wide_ref[z, 15:24] = pltpu.roll(rows[0:16], 288, 1)[6:15, 0:256]


def merge_kernel(own_ref, left_ref, right_ref, ah_ref, al_ref):
    for z in range(2):
        cells = [left_ref[0, z], left_ref[1, z]] + [own_ref[x, z] for x in range(4)]
        cells = cells + [right_ref[0, z], right_ref[1, z]]
        ah_ref[z], al_ref[z] = split(jnp.concatenate(cells, axis=0))


def views(near, far):
    lane = lanes(near.shape)
    return (
        pltpu.roll(jnp.where(lane >= 96, far, near), 32, 1),
        near,
        pltpu.roll(jnp.where(lane < 32, far, near), 96, 1),
        pltpu.roll(jnp.where(lane < 64, far, near), 64, 1),
    )


def product(high, low, kh_ref, kl_ref, z):
    kept = jnp.concatenate([h[48 * z : 48 * z + 192] for h in high], axis=0)
    rest = jnp.concatenate([h[48 * z : 48 * z + 192] for h in low], axis=0)
    both = dot(kh_ref[z], jnp.concatenate([kept, rest], axis=1))
    return own_lanes(both[:, 0:128] + both[:, 128:256] + dot(kl_ref[z], kept))


def gathered(own_ref, left_ref, right_ref):
    near = jnp.concatenate(
        [left_ref[:, 0:128], own_ref[0, :, 0:128], own_ref[1, :, 0:128], right_ref[0:96, 0:128]], axis=0
    )
    far = jnp.concatenate(
        [left_ref[:, 128:256], own_ref[0, :, 128:256], own_ref[1, :, 128:256], right_ref[0:96, 128:256]], axis=0
    )
    return views(near, far)


def sweep_kernel(top, own_ref, left_ref, right_ref, g_ref, ah_ref, al_ref, bh_ref, bl_ref, x_ref, rows, closed):
    seen = jnp.concatenate([left_ref[...], own_ref[0], own_ref[1], right_ref[0:96]], axis=0)
    look = [pltpu.roll(seen, 384 - 32 * start, 1)[:, 0:256] for start in (1, 2, 3, 4)]
    pairs = [split(view) for view in look]
    rows[24:32] = jnp.zeros((8, 256), F32)
    for z in range(2):
        kept = jnp.concatenate([p[0][48 * z : 48 * z + 192] for p in pairs], axis=0)
        rest = jnp.concatenate([p[1][48 * z : 48 * z + 192] for p in pairs], axis=0)
        both = dot(ah_ref[z], jnp.concatenate([kept, rest], axis=1))
        found = by_x(both[:, 0:256] + both[:, 256:512] + dot(al_ref[z], kept), 8, 24)
        rows[0:24] = g_ref[z] - found
        found = by_x(three(bh_ref[z], bl_ref[z], rows[...]), 8, 24)
        rows[0:24] = found
        at = 48 * z + 48
        body_rows = look[1][at : at + 16] + rows[0:16]
        body_rows = jnp.where(lax.broadcasted_iota(jnp.int32, (16, 256), 0) < 15, body_rows, 0.0)
        closed[...] = jnp.zeros((16, 256), F32)
        closed[6:15] = rows[15:24]
        after = look[2][at : at + 16] + closed[...]
        row = lax.broadcasted_iota(jnp.int32, (16, 256), 0)
        after = jnp.where((row >= 6) & (row < 15), after, 0.0)
        if top == 5:
            pad = jnp.zeros((16, 128), F32)
            body_rows = pltpu.roll(jnp.concatenate([body_rows, pad], axis=1), 64, 1)
            after = pltpu.roll(jnp.concatenate([after, pad], axis=1), 96, 1)
            x_ref[z] = jnp.where(lanes((16, 384)) // 32 == 10, after, body_rows)
        else:
            after = pltpu.roll(after, 32, 1)
            use = (lanes((16, 256)) // 32 == 7) & (row >= 6)
            x_ref[z] = pltpu.roll(jnp.where(use, after, body_rows), 192, 1)


def average_kernel(g_ref, right_ref, wide_ref, out_ref, ahead):
    for z in range(3):
        source = g_ref.at[z] if z < 2 else right_ref.at[96:112]
        ahead[z, 0:16] = source[:, 128:256]
        ahead[z, 16:32] = views(source[:, 128:256], source[:, 256:384])[2]
    for z in range(2):
        wide_ref[z] = jnp.zeros((48, 128), F32)
        for edge in range(12):
            ox, _, oz = OFFSETS[edge]
            start = 16 * ox + 3 * slot_of(edge)
            value = ahead[z + oz, start : start + 3]
            wide_ref[z, 3 * edge : 3 * edge + 3] = value
        write(out_ref, z, wide_ref[z, 0:36])


def write(out_ref, z, value):
    for x in range(4):
        out_ref[x, z] = value[:, 32 * x : 32 * x + 32]


def last_kernel(own_ref, left_ref, right_ref, wide_ref, ah_ref, al_ref, bh_ref, bl_ref, out_ref, rows, ahead, state):
    seen = gathered(own_ref, left_ref, right_ref)
    pairs = [split(view) for view in seen]
    high, low = [p[0] for p in pairs], [p[1] for p in pairs]
    state[...] = jnp.zeros((40, 128), F32)
    for z in range(3):
        ahead[z, 0:16] = seen[1][48 * z + 48 : 48 * z + 64]
        ahead[z, 16:32] = seen[2][48 * z + 48 : 48 * z + 64]
    for z in range(2):
        for edge in range(12):
            ox, _, oz = OFFSETS[edge]
            start = 16 * ox + 3 * slot_of(edge)
            state[3 * edge : 3 * edge + 3] = ahead[z + oz, start : start + 3]
        rows[...] = jnp.zeros((48, 128), F32)
        rows[0:36] = wide_ref[z, 0:36] - product(high, low, ah_ref, al_ref, z)[0:36]
        state[...] = state[...] + solve(bh_ref[z, :, 0:48], bl_ref[z, :, 0:48], rows)
        turned = state[...].T
        for x in range(4):
            out_ref[x, z] = turned[32 * x : 32 * x + 32, 0:36]


def after(value, *others):
    return lax.optimization_barrier((value, *others))[0]


def steps(displacement, dof_weight, coarse_matrix, block_inverse):
    weights = jnp.transpose(dof_weight[:, 0], (0, 2, 1, 3)).reshape(4, 24, 128)
    matrix = jnp.transpose(coarse_matrix[:, 0], (0, 2, 3, 1, 4)).reshape(4, 27, 72, 36)
    block = jnp.transpose(block_inverse[:, 0], (0, 2, 1, 3)).reshape(4, 72, 36)
    mine, ah, al, bh, bl, sent = start(displacement[:, 0], weights, block, matrix)
    left = shifted(mine, "gx", 1)
    right = shifted(mine, "gx", -1)
    rows_left = shifted(sent[2:4], "gx", 1)
    rows_right = shifted(sent[0:2], "gx", -1)
    sides = (mine, left, right)
    sums, up = call(sum_x_kernel, (shape(2, 32, 384), shape(24, 384)))(*sides)
    left = shifted(up, "gz", 1)
    lower, upper, middle = call(sum_z_kernel, (shape(2, 8, 384),) * 3)(sums, left)
    below = shifted(upper, "gy", 1)
    above = shifted(lower, "gy", -1)
    g, near, x, near_high, near_low = call(
        first_kernel,
        (shape(2, 16, 384), shape(2, 24, 256), shape(2, 16, 384)) + (shape(2, 192, 32, dtype=BF16),) * 2,
        (pltpu.VMEM((32, 384), F32),),
    )(lower, upper, middle, below, above, *sides)
    for sweep in range(3):
        below = shifted(x, "gy", 1)
        above = shifted(x, "gy", -1)
        if sweep == 0:
            rows_left = after(rows_left, below, above)
            wide = (shape(2, 192, 768, dtype=BF16),) * 2
            operator = call(merge_kernel, wide, flops=10_000_000)(sent, rows_left, rows_right)
        own = jnp.concatenate([x, below, above], axis=1)
        left = shifted(own[1], "gz", 1)
        moving = own.reshape(96, own.shape[2])
        if sweep == 0:
            moving = jnp.concatenate([moving, g[0]], axis=0)
        right = shifted(moving, "gz", -1)
        if sweep == 0:
            every, average = call(
                average_kernel, (shape(2, 48, 128), shape(4, 2, 36, 32)), (pltpu.VMEM((3, 32, 128), F32),)
            )(g, right)
        if sweep < 2:
            x = call(
                functools.partial(sweep_kernel, 5 - sweep),
                shape(2, 16, 384 if sweep == 0 else 256),
                (pltpu.VMEM((32, 256), F32), pltpu.VMEM((16, 256), F32)),
                flops=20_000_000,
            )(own, left, right, near, *operator, near_high, near_low)
    x = call(
        last_kernel,
        shape(4, 2, 32, 36),
        (pltpu.VMEM((48, 128), F32), pltpu.VMEM((3, 32, 128), F32), pltpu.VMEM((40, 128), F32)),
        flops=10_000_000,
    )(own, left, right, every, ah, al, bh, bl)
    return average.reshape(4, 1, 2, 12, 3, 32), jnp.swapaxes(x, 2, 3)[:, None]


def solution(mesh):
    placed = (
        P("gx", "gy", "gz", None, None, None, None),
        P("gx", "gy", "gz", None, None),
        P("gx", "gy", "gz", None, None, None),
        P("gx", "gy", "gz", None, None),
    )
    return jax.shard_map(
        steps,
        mesh=mesh,
        in_specs=placed,
        out_specs=(P("gx", "gy", "gz", None, None, None), P("gx", "gy", "gz", None, None)),
        check_vma=False,
    )
```

```python
import functools

import jax
import jax.numpy as jnp
import numpy as np
from jax import lax
from jax.experimental import pallas as pl
from jax.experimental.pallas import tpu as pltpu
from jax.sharding import PartitionSpec as P


F32 = jnp.float32
BF16 = jnp.bfloat16
OFFSETS = (
    (0, 0, 0), (0, 0, 1), (0, 1, 0), (0, 1, 1),
    (0, 0, 0), (0, 0, 1), (1, 0, 0), (1, 0, 1),
    (0, 0, 0), (0, 1, 0), (1, 0, 0), (1, 1, 0),
)
WIDE_EDGES = (0, 2, 4, 8, 9, 6, 10, 11)


def slot_of(edge):
    direction = edge // 4
    upper = OFFSETS[edge][1]
    return (0 + upper, 2, 3 + upper)[direction]


def placement():
    table = np.zeros((384, 384), np.float32)
    for offset in range(9):
        dy, dz = offset // 3 - 1, offset % 3 - 1
        for edge in range(12):
            ox, oy, oz = OFFSETS[edge]
            direction = edge // 4
            if direction == 1:
                group, slot = {-1: (1, 2), 0: (0, 2), 1: (2, 2)}[dy + oy]
            else:
                base = 0 if direction == 0 else 3
                group, slot = {-1: (1, base), 0: (0, base), 1: (0, base + 1), 2: (2, base + 1)}[dy + oy]
            for comp in range(3):
                row = 16 * group + 3 * slot + comp
                table[36 * offset + 3 * edge + comp, 192 * ox + 48 * (dz + oz + 1) + row] = 1.0
    return table


def choice():
    table = np.zeros((512, 128), np.float32)
    for x in range(4):
        for place, edge in enumerate(WIDE_EDGES):
            for comp in range(3):
                table[128 * x + 3 * edge + comp, 32 * x + 3 * place + comp] = 1.0
    return table


def shifted(block, axis, distance):
    count = lax.axis_size(axis)
    return lax.ppermute(block, axis, [((i - distance) % count, i) for i in range(count)])


def matched(block, axis, which):
    count = lax.axis_size(axis)
    return lax.ppermute(block, axis, [(i, (i - 1 if i % 2 == which else i + 1) % count) for i in range(count)])


def ordered(even, pair):
    return jnp.where(even, pair[0], pair[1]), jnp.where(even, pair[1], pair[0])


def lanes(shape):
    return lax.broadcasted_iota(jnp.int32, shape, len(shape) - 1)


def split(value):
    high = value.astype(BF16)
    return high, (value - high.astype(F32)).astype(BF16)


def dot(a, b):
    return jnp.dot(a, b, preferred_element_type=F32)


def own_lanes(value):
    group = lanes((40, 128)) // 32
    total = jnp.where(group == 0, value[0:40], 0.0)
    for x in range(1, 4):
        total = total + jnp.where(group == x, value[40 * x : 40 * x + 40], 0.0)
    return total


def call(kernel, outs, scratch=(), flops=1_000_000, scalar=False, count=0, **options):
    if scalar:
        places = [pltpu.SMEM] + [pltpu.VMEM] * count
        options["in_specs"] = [pl.BlockSpec(memory_space=place) for place in places]
    return pl.pallas_call(
        kernel,
        out_shape=outs,
        scratch_shapes=list(scratch),
        cost_estimate=pl.CostEstimate(flops=flops, bytes_accessed=1_000_000, transcendentals=0),
        compiler_params=pltpu.CompilerParams(vmem_limit_bytes=40 * 1024 * 1024),
        **options,
    )


def streamed(*arrays):
    return [pltpu.with_memory_space_constraint(a, pltpu.HBM) for a in arrays]


def shape(*dims, dtype=F32):
    return jax.ShapeDtypeStruct(dims, dtype)


def pick(rows_ref, value):
    rows_ref[...] = value
    return [rows_ref[3 * edge : 3 * edge + 3] for edge in WIDE_EDGES]


def take_sums(step, disp_ref, weights, held):
    ones = jnp.ones((128, 128), BF16)
    group = (lanes((4, 512)) % 128) // 32
    keep = group == lax.broadcasted_iota(jnp.int32, (4, 512), 0)
    for z in range(2):
        pieces = []
        for edge in range(3):
            parts = [disp_ref[x, z, edge, c] for c in range(3) for x in range(4)]
            right = jnp.concatenate(parts + [ones], axis=0)
            at = 6 * step + 2 * edge + z
            left = jnp.concatenate([weights[x, pl.ds(at, 1), :] for x in range(4)], axis=0).astype(BF16)
            found = lax.dot_general(left, right, (((1,), (1,)), ((), ())), preferred_element_type=F32)
            row = jnp.sum(jnp.where(keep, found, 0.0), axis=0, keepdims=True)
            pieces = pieces + [row[:, 128 * c : 128 * c + 128] for c in range(4)]
        held[step, z, 0:12] = jnp.concatenate(pieces, axis=0)


def take_operator(matrix_ref, place_ref, ah_ref, al_ref, sent_ref, packed, stacked, full):
    for offset in range(27):
        start, tile = 36 * (offset % 9) % 128, 3 * (offset // 9) + 36 * (offset % 9) // 128
        size = min(36, 128 - start)
        packed[tile, :, start : start + size] = matrix_ref[0, offset, :, 0:size]
        if size < 36:
            packed[tile + 1, :, 0 : 36 - size] = matrix_ref[0, offset, :, size:36]
    pad = jnp.zeros((4, 384), BF16)
    found = []
    for dx in range(3):
        for z in range(2):
            high, low = split(
                jnp.concatenate([packed[3 * dx + k, pl.ds(z, 36, stride=2), :] for k in range(3)], axis=1)
            )
            stacked[40 * z : 40 * z + 40] = jnp.concatenate([high, pad], axis=0)
            stacked[80 + 40 * z : 120 + 40 * z] = jnp.concatenate([low, pad], axis=0)
        found.append(dot(stacked[...], place_ref[...]))
    none = jnp.zeros((160, 384), F32)
    total = jnp.concatenate([found[0], found[2]], axis=1)
    total = total + pltpu.roll(jnp.concatenate([found[1], none], axis=1), 192, 1)
    for z in range(2):
        high, low = total[40 * z : 40 * z + 40], total[80 + 40 * z : 120 + 40 * z]
        ah_ref[z, 0] = high.astype(BF16)
        al_ref[z, 0] = low.astype(BF16)
        for place, value in enumerate(pick(full, high + low)):
            sent_ref[0, z, 3 * place : 3 * place + 3] = value


def start_kernel(
    disp_ref, weight_ref, block_ref, choice_ref, matrix_ref, place_ref,
    sums_ref, ah_ref, al_ref, bh_ref, bl_ref, sent_ref,
    weights, inner, rows, held, packed, stacked, full,
):
    step = pl.program_id(0)

    @pl.when(step == 0)
    def _():
        weights[...] = weight_ref[...].astype(F32)
        inner[...] = jnp.zeros((4, 72, 128), F32)
        for tile in range(9):
            packed[tile] = jnp.zeros((72, 128), F32)
        for x in range(4):
            inner[x, :, 0:36] = block_ref[x]
        for z in range(2):
            value = jnp.concatenate([inner[x, pl.ds(z, 36, stride=2), :] for x in range(4)], axis=1)
            high, low = split(value)
            rows[0:36] = dot(high, choice_ref[...]) + dot(low, choice_ref[...])
            for place, edge in enumerate(WIDE_EDGES):
                sums_ref[z, 48 + 3 * place : 51 + 3 * place] = rows[3 * edge : 3 * edge + 3]

    take_sums(step, disp_ref, weights, held)
    take_operator(matrix_ref, place_ref, ah_ref, al_ref, sent_ref, packed, stacked, full)
    for z in range(2):
        high, low = split(inner[step, pl.ds(z, 36, stride=2), :])
        pad = jnp.zeros((4, 128), BF16)
        bh_ref[z, 0] = jnp.concatenate([high, pad], axis=0)
        bl_ref[z, 0] = jnp.concatenate([low, pad], axis=0)

    @pl.when(step == 3)
    def _():
        for z in range(2):
            for part in range(4):
                sums_ref[z, 12 * part : 12 * part + 12] = held[part, z, 0:12]


def start(displacement, weights, block, matrix):
    outs = (shape(2, 72, 128),) + (shape(2, 4, 40, 768, dtype=BF16),) * 2
    outs = outs + (shape(2, 4, 40, 128, dtype=BF16),) * 2 + (shape(4, 2, 24, 768),)
    wide = pl.BlockSpec((2, 1, 40, 768), lambda i: (0, i, 0, 0))
    slim = pl.BlockSpec((2, 1, 40, 128), lambda i: (0, i, 0, 0))
    sums, ah, al, bh, bl, sent = call(
        start_kernel,
        outs,
        (
            pltpu.VMEM((4, 24, 128), F32),
            pltpu.VMEM((4, 72, 128), F32),
            pltpu.VMEM((40, 128), F32),
            pltpu.VMEM((4, 2, 16, 128), F32),
            pltpu.VMEM((9, 72, 128), F32),
            pltpu.VMEM((160, 384), BF16),
            pltpu.VMEM((40, 768), F32),
        ),
        flops=40_000_000,
        grid=(4,),
        in_specs=[
            pl.BlockSpec((4, 2, 3, 3, 32, 128), lambda i: (0, 0, i, 0, 0, 0)),
            pl.BlockSpec((4, 24, 128), lambda i: (0, 0, 0)),
            pl.BlockSpec((4, 72, 36), lambda i: (0, 0, 0)),
            pl.BlockSpec((512, 128), lambda i: (0, 0)),
            pl.BlockSpec((1, 27, 72, 36), lambda i: (i, 0, 0, 0)),
            pl.BlockSpec((384, 384), lambda i: (0, 0)),
        ],
        out_specs=(
            pl.BlockSpec((2, 72, 128), lambda i: (0, 0, 0)),
            wide,
            wide,
            slim,
            slim,
            pl.BlockSpec((1, 2, 24, 768), lambda i: (i, 0, 0, 0)),
        ),
    )(*streamed(displacement, weights, block, jnp.asarray(choice(), BF16), matrix, jnp.asarray(placement(), BF16)))
    return (
        sums, ah.reshape(2, 160, 768), al.reshape(2, 160, 768),
        bh.reshape(2, 160, 128), bl.reshape(2, 160, 128), sent,
    )


def sum_x_kernel(sums_ref, left_ref, right_ref, out_ref, up_ref):
    for z in range(2):
        all_x = jnp.concatenate([left_ref[z, 0:48], sums_ref[z, 0:48], right_ref[z, 0:48]], axis=1)
        below = pltpu.roll(all_x, 32, 1)
        out_ref[z, 0:16] = all_x[0:16]
        out_ref[z, 16:24] = all_x[16:24] + below[24:32]
        out_ref[z, 24:32] = all_x[32:40] + below[40:48]
    up_ref[...] = out_ref[1, 0:24]


def sum_z_kernel(sums_ref, left_ref, lower_ref, upper_ref, middle_ref):
    for z in range(2):
        below = left_ref if z == 0 else sums_ref.at[0]
        lower_ref[z, 0:4] = sums_ref[z, 0:4] + below[4:8]
        lower_ref[z, 4:8] = sums_ref[z, 24:28]
        upper_ref[z, 0:4] = sums_ref[z, 8:12] + below[12:16]
        upper_ref[z, 4:8] = sums_ref[z, 28:32]
        middle_ref[z, 0:4] = sums_ref[z, 16:20] + below[20:24]
        middle_ref[z, 4:8] = sums_ref[z, 16:20]


def by_x(value, count, rows):
    group = lanes((rows, value.shape[1])) // 32
    total = jnp.where(group == 0, value[0:rows], 0.0)
    for x in range(1, count):
        total = total + jnp.where(group == x, value[rows * x : rows * x + rows], 0.0)
    return total


def three(high, low, value):
    kept, rest = split(value)
    return dot(high, kept) + dot(high, rest) + dot(low, kept)


def solve(block_high, block_low, rows_ref):
    return own_lanes(three(block_high, block_low, rows_ref[...]))


def first_kernel(
    lower_ref, upper_ref, middle_ref, below_ref, above_ref, own_ref, left_ref, right_ref,
    g_ref, wide_ref, x_ref, bh_ref, bl_ref, rows,
):
    for z in range(2):
        rows[...] = jnp.zeros((32, 384), F32)
        node = lower_ref[z] + below_ref[z]
        top = upper_ref[z] + above_ref[z]
        middle = middle_ref[z]
        for slot, (source, at) in enumerate(((node, 0), (top, 0), (middle, 0), (node, 4), (top, 4))):
            rows[3 * slot : 3 * slot + 3] = source[at : at + 3] / source[at + 3 : at + 4]
        parts = [ref[z, 48:72, 32 * x : 32 * x + 32] for ref in (left_ref, own_ref, right_ref) for x in range(4)]
        high, low = split(jnp.concatenate(parts, axis=0))
        bh_ref[z], bl_ref[z] = high[48:240], low[48:240]
        found = by_x(three(high, low, rows[...]), 12, 24)
        x_ref[z] = jnp.where(lax.broadcasted_iota(jnp.int32, (16, 384), 0) < 15, found[0:16], 0.0)
        g_ref[z] = rows[0:16]
        wide_ref[z, 0:16] = pltpu.roll(rows[0:16], 320, 1)[:, 0:256]
        wide_ref[z, 15:24] = pltpu.roll(rows[0:16], 288, 1)[6:15, 0:256]


def merge_kernel(own_ref, left_ref, right_ref, ah_ref, al_ref):
    for z in range(2):
        cells = [left_ref[0, z], left_ref[1, z]] + [own_ref[x, z] for x in range(4)]
        cells = cells + [right_ref[0, z], right_ref[1, z]]
        ah_ref[z], al_ref[z] = split(jnp.concatenate(cells, axis=0))


def views(near, far):
    lane = lanes(near.shape)
    return (
        pltpu.roll(jnp.where(lane >= 96, far, near), 32, 1),
        near,
        pltpu.roll(jnp.where(lane < 32, far, near), 96, 1),
        pltpu.roll(jnp.where(lane < 64, far, near), 64, 1),
    )


def product(high, low, kh_ref, kl_ref, z):
    kept = jnp.concatenate([h[48 * z : 48 * z + 192] for h in high], axis=0)
    rest = jnp.concatenate([h[48 * z : 48 * z + 192] for h in low], axis=0)
    both = dot(kh_ref[z], jnp.concatenate([kept, rest], axis=1))
    return own_lanes(both[:, 0:128] + both[:, 128:256] + dot(kl_ref[z], kept))


def gathered(odd_ref, own_ref, first_ref, second_ref):
    left, right = sides_of(odd_ref, first_ref, second_ref)
    all_z = jnp.concatenate([left, own_ref[0], own_ref[1], right], axis=0)
    return views(all_z[:, 0:128], all_z[:, 128:256])


def sides_of(odd_ref, first_ref, second_ref):
    odd = jnp.full(first_ref.shape, odd_ref[0], jnp.int32) == 1
    return jnp.where(odd[48:96], second_ref[48:96], first_ref[48:96]), jnp.where(odd, first_ref[...], second_ref[...])


def sweep_kernel(top, odd_ref, own_ref, first_ref, second_ref, g_ref, ah_ref, al_ref, bh_ref, bl_ref, x_ref, rows, closed):
    left, right = sides_of(odd_ref, first_ref, second_ref)
    seen = jnp.concatenate([left, own_ref[0], own_ref[1], right[0:96]], axis=0)
    look = [pltpu.roll(seen, 384 - 32 * start, 1)[:, 0:256] for start in (1, 2, 3, 4)]
    pairs = [split(view) for view in look]
    rows[24:32] = jnp.zeros((8, 256), F32)
    for z in range(2):
        kept = jnp.concatenate([p[0][48 * z : 48 * z + 192] for p in pairs], axis=0)
        rest = jnp.concatenate([p[1][48 * z : 48 * z + 192] for p in pairs], axis=0)
        both = dot(ah_ref[z], jnp.concatenate([kept, rest], axis=1))
        found = by_x(both[:, 0:256] + both[:, 256:512] + dot(al_ref[z], kept), 8, 24)
        rows[0:24] = g_ref[z] - found
        found = by_x(three(bh_ref[z], bl_ref[z], rows[...]), 8, 24)
        rows[0:24] = found
        at = 48 * z + 48
        body_rows = look[1][at : at + 16] + rows[0:16]
        body_rows = jnp.where(lax.broadcasted_iota(jnp.int32, (16, 256), 0) < 15, body_rows, 0.0)
        closed[...] = jnp.zeros((16, 256), F32)
        closed[6:15] = rows[15:24]
        after = look[2][at : at + 16] + closed[...]
        row = lax.broadcasted_iota(jnp.int32, (16, 256), 0)
        after = jnp.where((row >= 6) & (row < 15), after, 0.0)
        if top == 5:
            pad = jnp.zeros((16, 128), F32)
            body_rows = pltpu.roll(jnp.concatenate([body_rows, pad], axis=1), 64, 1)
            after = pltpu.roll(jnp.concatenate([after, pad], axis=1), 96, 1)
            x_ref[z] = jnp.where(lanes((16, 384)) // 32 == 10, after, body_rows)
        else:
            after = pltpu.roll(after, 32, 1)
            use = (lanes((16, 256)) // 32 == 7) & (row >= 6)
            x_ref[z] = pltpu.roll(jnp.where(use, after, body_rows), 192, 1)


def average_kernel(odd_ref, g_ref, first_ref, second_ref, wide_ref, out_ref, ahead):
    for z in range(3):
        source = g_ref[z] if z < 2 else sides_of(odd_ref, first_ref, second_ref)[1][96:112]
        ahead[z, 0:16] = source[:, 128:256]
        ahead[z, 16:32] = views(source[:, 128:256], source[:, 256:384])[2]
    for z in range(2):
        wide_ref[z] = jnp.zeros((48, 128), F32)
        for edge in range(12):
            ox, _, oz = OFFSETS[edge]
            start = 16 * ox + 3 * slot_of(edge)
            value = ahead[z + oz, start : start + 3]
            wide_ref[z, 3 * edge : 3 * edge + 3] = value
        write(out_ref, z, wide_ref[z, 0:36])


def write(out_ref, z, value):
    for x in range(4):
        out_ref[x, z] = value[:, 32 * x : 32 * x + 32]


def last_kernel(
    odd_ref, own_ref, first_ref, second_ref, wide_ref, ah_ref, al_ref, bh_ref, bl_ref, out_ref, rows, ahead, state
):
    seen = gathered(odd_ref, own_ref, first_ref, second_ref)
    pairs = [split(view) for view in seen]
    high, low = [p[0] for p in pairs], [p[1] for p in pairs]
    state[...] = jnp.zeros((40, 128), F32)
    for z in range(3):
        ahead[z, 0:16] = seen[1][48 * z + 48 : 48 * z + 64]
        ahead[z, 16:32] = seen[2][48 * z + 48 : 48 * z + 64]
    for z in range(2):
        for edge in range(12):
            ox, _, oz = OFFSETS[edge]
            start = 16 * ox + 3 * slot_of(edge)
            state[3 * edge : 3 * edge + 3] = ahead[z + oz, start : start + 3]
        rows[...] = jnp.zeros((48, 128), F32)
        rows[0:36] = wide_ref[z, 0:36] - product(high, low, ah_ref, al_ref, z)[0:36]
        state[...] = state[...] + solve(bh_ref[z, :, 0:48], bl_ref[z, :, 0:48], rows)
        turned = state[...].T
        for x in range(4):
            out_ref[x, z] = turned[32 * x : 32 * x + 32, 0:36]


def after(value, *others):
    return lax.optimization_barrier((value, *others))[0]


def steps(displacement, dof_weight, coarse_matrix, block_inverse):
    weights = jnp.transpose(dof_weight[:, 0], (0, 2, 1, 3)).reshape(4, 24, 128)
    matrix = jnp.transpose(coarse_matrix[:, 0], (0, 2, 3, 1, 4)).reshape(4, 27, 72, 36)
    block = jnp.transpose(block_inverse[:, 0], (0, 2, 1, 3)).reshape(4, 72, 36)
    mine, ah, al, bh, bl, sent = start(displacement[:, 0], weights, block, matrix)
    left = shifted(mine, "gx", 1)
    right = shifted(mine, "gx", -1)
    rows_left = shifted(sent[2:4], "gx", 1)
    rows_right = shifted(sent[0:2], "gx", -1)
    sides = (mine, left, right)
    sums, up = call(sum_x_kernel, (shape(2, 32, 384), shape(24, 384)))(*sides)
    left = shifted(up, "gz", 1)
    lower, upper, middle = call(sum_z_kernel, (shape(2, 8, 384),) * 3)(sums, left)
    even = lax.axis_index("gy") % 2 == 0
    odd = (lax.axis_index("gz") % 2).astype(jnp.int32).reshape(1)
    sent_down, sent_up = ordered(even, (lower, upper))
    pair = []
    for which, value in enumerate((sent_down, sent_up)):
        pair.append(matched(value, "gy", which))
    below, above = ordered(even, pair)
    g, near, x, near_high, near_low = call(
        first_kernel,
        (shape(2, 16, 384), shape(2, 24, 256), shape(2, 16, 384)) + (shape(2, 192, 32, dtype=BF16),) * 2,
        (pltpu.VMEM((32, 384), F32),),
    )(lower, upper, middle, below, above, *sides)
    for sweep in range(3):
        pair = []
        for which in range(2):
            pair.append(matched(x, "gy", which))
        if sweep == 0:
            rows_left = after(rows_left, *pair)
            wide = (shape(2, 192, 768, dtype=BF16),) * 2
            operator = call(merge_kernel, wide, flops=10_000_000)(sent, rows_left, rows_right)
        own = jnp.concatenate([x, *ordered(even, pair)], axis=1)
        moving = own.reshape(96, own.shape[2])
        if sweep == 0:
            moving = jnp.concatenate([moving, g[0]], axis=0)
        pair = []
        for which in range(2):
            pair.append(matched(moving, "gz", which))
        if sweep == 0:
            every, average = call(
                average_kernel,
                (shape(2, 48, 128), shape(4, 2, 36, 32)),
                (pltpu.VMEM((3, 32, 128), F32),),
                scalar=True,
                count=3,
            )(odd, g, *pair)
        if sweep < 2:
            x = call(
                functools.partial(sweep_kernel, 5 - sweep),
                shape(2, 16, 384 if sweep == 0 else 256),
                (pltpu.VMEM((32, 256), F32), pltpu.VMEM((16, 256), F32)),
                flops=20_000_000,
                scalar=True,
                count=8,
            )(odd, own, *pair, near, *operator, near_high, near_low)
    x = call(
        last_kernel,
        shape(4, 2, 32, 36),
        (pltpu.VMEM((48, 128), F32), pltpu.VMEM((3, 32, 128), F32), pltpu.VMEM((40, 128), F32)),
        flops=10_000_000,
        scalar=True,
        count=8,
    )(odd, own, *pair, every, ah, al, bh, bl)
    return average.reshape(4, 1, 2, 12, 3, 32), jnp.swapaxes(x, 2, 3)[:, None]


def solution(mesh):
    placed = (
        P("gx", "gy", "gz", None, None, None, None),
        P("gx", "gy", "gz", None, None),
        P("gx", "gy", "gz", None, None, None),
        P("gx", "gy", "gz", None, None),
    )
    return jax.shard_map(
        steps,
        mesh=mesh,
        in_specs=placed,
        out_specs=(P("gx", "gy", "gz", None, None, None), P("gx", "gy", "gz", None, None)),
        check_vma=False,
    )
```

```python
import functools

import jax
import jax.numpy as jnp
import numpy as np
from jax import lax
from jax.experimental import pallas as pl
from jax.experimental.pallas import tpu as pltpu
from jax.sharding import PartitionSpec as P


F32 = jnp.float32
BF16 = jnp.bfloat16
OFFSETS = (
    (0, 0, 0), (0, 0, 1), (0, 1, 0), (0, 1, 1),
    (0, 0, 0), (0, 0, 1), (1, 0, 0), (1, 0, 1),
    (0, 0, 0), (0, 1, 0), (1, 0, 0), (1, 1, 0),
)
WIDE_EDGES = (0, 2, 4, 8, 9, 6, 10, 11)


def slot_of(edge):
    direction = edge // 4
    upper = OFFSETS[edge][1]
    return (0 + upper, 2, 3 + upper)[direction]


def placement():
    table = np.zeros((384, 384), np.float32)
    for offset in range(9):
        dy, dz = offset // 3 - 1, offset % 3 - 1
        for edge in range(12):
            ox, oy, oz = OFFSETS[edge]
            direction = edge // 4
            if direction == 1:
                group, slot = {-1: (1, 2), 0: (0, 2), 1: (2, 2)}[dy + oy]
            else:
                base = 0 if direction == 0 else 3
                group, slot = {-1: (1, base), 0: (0, base), 1: (0, base + 1), 2: (2, base + 1)}[dy + oy]
            for comp in range(3):
                row = 16 * group + 3 * slot + comp
                table[36 * offset + 3 * edge + comp, 192 * ox + 48 * (dz + oz + 1) + row] = 1.0
    return table


def choice():
    table = np.zeros((512, 128), np.float32)
    for x in range(4):
        for place, edge in enumerate(WIDE_EDGES):
            for comp in range(3):
                table[128 * x + 3 * edge + comp, 32 * x + 3 * place + comp] = 1.0
    return table


def shifted(block, axis, distance):
    count = lax.axis_size(axis)
    return lax.ppermute(block, axis, [((i - distance) % count, i) for i in range(count)])


def matched(block, axis, which):
    count = lax.axis_size(axis)
    return lax.ppermute(block, axis, [(i, (i - 1 if i % 2 == which else i + 1) % count) for i in range(count)])


def ordered(even, pair):
    return jnp.where(even, pair[0], pair[1]), jnp.where(even, pair[1], pair[0])


def lanes(shape):
    return lax.broadcasted_iota(jnp.int32, shape, len(shape) - 1)


def split(value):
    high = value.astype(BF16)
    return high, (value - high.astype(F32)).astype(BF16)


def dot(a, b):
    return jnp.dot(a, b, preferred_element_type=F32)


def own_lanes(value):
    group = lanes((40, 128)) // 32
    total = jnp.where(group == 0, value[0:40], 0.0)
    for x in range(1, 4):
        total = total + jnp.where(group == x, value[40 * x : 40 * x + 40], 0.0)
    return total


def call(kernel, outs, scratch=(), flops=1_000_000, scalar=False, count=0, **options):
    if scalar:
        places = [pltpu.SMEM] + [pltpu.VMEM] * count
        options["in_specs"] = [pl.BlockSpec(memory_space=place) for place in places]
    return pl.pallas_call(
        kernel,
        out_shape=outs,
        scratch_shapes=list(scratch),
        cost_estimate=pl.CostEstimate(flops=flops, bytes_accessed=1_000_000, transcendentals=0),
        compiler_params=pltpu.CompilerParams(vmem_limit_bytes=40 * 1024 * 1024),
        **options,
    )


def streamed(*arrays):
    return [pltpu.with_memory_space_constraint(a, pltpu.HBM) for a in arrays]


def shape(*dims, dtype=F32):
    return jax.ShapeDtypeStruct(dims, dtype)


def take_sums(step, disp_ref, weights, held):
    ones = jnp.ones((128, 128), BF16)
    group = (lanes((4, 512)) % 128) // 32
    keep = group == lax.broadcasted_iota(jnp.int32, (4, 512), 0)
    for z in range(2):
        pieces = []
        for edge in range(3):
            parts = [disp_ref[x, z, edge, c] for c in range(3) for x in range(4)]
            right = jnp.concatenate(parts + [ones], axis=0)
            at = 6 * step + 2 * edge + z
            left = jnp.concatenate([weights[x, pl.ds(at, 1), :] for x in range(4)], axis=0).astype(BF16)
            found = lax.dot_general(left, right, (((1,), (1,)), ((), ())), preferred_element_type=F32)
            row = jnp.sum(jnp.where(keep, found, 0.0), axis=0, keepdims=True)
            pieces = pieces + [row[:, 128 * c : 128 * c + 128] for c in range(4)]
        held[step, z, 0:12] = jnp.concatenate(pieces, axis=0)


def take_operator(step, matrix_ref, place_ref, ah_ref, al_ref, halves, packed, stacked, full):
    for offset in range(27):
        start, tile = 36 * (offset % 9) % 128, 3 * (offset // 9) + 36 * (offset % 9) // 128
        size = min(36, 128 - start)
        packed[tile, :, start : start + size] = matrix_ref[0, offset, :, 0:size]
        if size < 36:
            packed[tile + 1, :, 0 : 36 - size] = matrix_ref[0, offset, :, size:36]
    pad = jnp.zeros((4, 384), BF16)
    found = []
    for dx in range(3):
        for z in range(2):
            high, low = split(
                jnp.concatenate([packed[3 * dx + k, pl.ds(z, 36, stride=2), :] for k in range(3)], axis=1)
            )
            stacked[40 * z : 40 * z + 40] = jnp.concatenate([high, pad], axis=0)
            stacked[80 + 40 * z : 120 + 40 * z] = jnp.concatenate([low, pad], axis=0)
        found.append(dot(stacked[...], place_ref[...]))
    none = jnp.zeros((160, 384), F32)
    total = jnp.concatenate([found[0], found[2]], axis=1)
    total = total + pltpu.roll(jnp.concatenate([found[1], none], axis=1), 192, 1)
    for z in range(2):
        high, low = total[40 * z : 40 * z + 40], total[80 + 40 * z : 120 + 40 * z]
        ah_ref[z, 0] = high.astype(BF16)
        al_ref[z, 0] = low.astype(BF16)
        full[...] = high + low
        for half, half_ref in enumerate(halves):

            @pl.when(step // 2 == half)
            def _(half_ref=half_ref, z=z):
                for place, edge in enumerate(WIDE_EDGES):
                    half_ref[0, z, 3 * place : 3 * place + 3] = full[3 * edge : 3 * edge + 3]


def start_kernel(
    disp_ref, weight_ref, block_ref, choice_ref, matrix_ref, place_ref,
    sums_ref, ah_ref, al_ref, bh_ref, bl_ref, near_ref, far_ref,
    weights, inner, rows, held, packed, stacked, full,
):
    step = pl.program_id(0)

    @pl.when(step == 0)
    def _():
        weights[...] = weight_ref[...].astype(F32)
        inner[...] = jnp.zeros((4, 72, 128), F32)
        for tile in range(9):
            packed[tile] = jnp.zeros((72, 128), F32)
        for x in range(4):
            inner[x, :, 0:36] = block_ref[x]
        for z in range(2):
            value = jnp.concatenate([inner[x, pl.ds(z, 36, stride=2), :] for x in range(4)], axis=1)
            high, low = split(value)
            rows[0:36] = dot(high, choice_ref[...]) + dot(low, choice_ref[...])
            for place, edge in enumerate(WIDE_EDGES):
                sums_ref[z, 48 + 3 * place : 51 + 3 * place] = rows[3 * edge : 3 * edge + 3]

    take_sums(step, disp_ref, weights, held)
    take_operator(step, matrix_ref, place_ref, ah_ref, al_ref, (near_ref, far_ref), packed, stacked, full)
    for z in range(2):
        high, low = split(inner[step, pl.ds(z, 36, stride=2), :])
        pad = jnp.zeros((4, 128), BF16)
        bh_ref[z, 0] = jnp.concatenate([high, pad], axis=0)
        bl_ref[z, 0] = jnp.concatenate([low, pad], axis=0)

    @pl.when(step == 3)
    def _():
        for z in range(2):
            for part in range(4):
                sums_ref[z, 12 * part : 12 * part + 12] = held[part, z, 0:12]


def start(displacement, weights, block, matrix):
    outs = (shape(2, 72, 128),) + (shape(2, 4, 40, 768, dtype=BF16),) * 2
    outs = outs + (shape(2, 4, 40, 128, dtype=BF16),) * 2 + (shape(2, 2, 24, 768),) * 2
    wide = pl.BlockSpec((2, 1, 40, 768), lambda i: (0, i, 0, 0))
    slim = pl.BlockSpec((2, 1, 40, 128), lambda i: (0, i, 0, 0))
    sums, ah, al, bh, bl, near, far = call(
        start_kernel,
        outs,
        (
            pltpu.VMEM((4, 24, 128), F32),
            pltpu.VMEM((4, 72, 128), F32),
            pltpu.VMEM((40, 128), F32),
            pltpu.VMEM((4, 2, 16, 128), F32),
            pltpu.VMEM((9, 72, 128), F32),
            pltpu.VMEM((160, 384), BF16),
            pltpu.VMEM((40, 768), F32),
        ),
        flops=40_000_000,
        grid=(4,),
        in_specs=[
            pl.BlockSpec((4, 2, 3, 3, 32, 128), lambda i: (0, 0, i, 0, 0, 0)),
            pl.BlockSpec((4, 24, 128), lambda i: (0, 0, 0)),
            pl.BlockSpec((4, 72, 36), lambda i: (0, 0, 0)),
            pl.BlockSpec((512, 128), lambda i: (0, 0)),
            pl.BlockSpec((1, 27, 72, 36), lambda i: (i, 0, 0, 0)),
            pl.BlockSpec((384, 384), lambda i: (0, 0)),
        ],
        out_specs=(
            pl.BlockSpec((2, 72, 128), lambda i: (0, 0, 0)),
            wide,
            wide,
            slim,
            slim,
            pl.BlockSpec((1, 2, 24, 768), lambda i: (jnp.minimum(i, 1), 0, 0, 0)),
            pl.BlockSpec((1, 2, 24, 768), lambda i: (jnp.maximum(i - 2, 0), 0, 0, 0)),
        ),
    )(*streamed(displacement, weights, block, jnp.asarray(choice(), BF16), matrix, jnp.asarray(placement(), BF16)))
    return (
        sums, ah.reshape(2, 160, 768), al.reshape(2, 160, 768),
        bh.reshape(2, 160, 128), bl.reshape(2, 160, 128), near, far,
    )


def sum_x_kernel(sums_ref, left_ref, right_ref, out_ref, up_ref):
    for z in range(2):
        all_x = jnp.concatenate([left_ref[z, 0:48], sums_ref[z, 0:48], right_ref[z, 0:48]], axis=1)
        below = pltpu.roll(all_x, 32, 1)
        out_ref[z, 0:16] = all_x[0:16]
        out_ref[z, 16:24] = all_x[16:24] + below[24:32]
        out_ref[z, 24:32] = all_x[32:40] + below[40:48]
    up_ref[...] = out_ref[1, 0:24]


def sum_z_kernel(sums_ref, left_ref, lower_ref, upper_ref, middle_ref):
    for z in range(2):
        below = left_ref if z == 0 else sums_ref.at[0]
        lower_ref[z, 0:4] = sums_ref[z, 0:4] + below[4:8]
        lower_ref[z, 4:8] = sums_ref[z, 24:28]
        upper_ref[z, 0:4] = sums_ref[z, 8:12] + below[12:16]
        upper_ref[z, 4:8] = sums_ref[z, 28:32]
        middle_ref[z, 0:4] = sums_ref[z, 16:20] + below[20:24]
        middle_ref[z, 4:8] = sums_ref[z, 16:20]


def by_x(value, count, rows):
    group = lanes((rows, value.shape[1])) // 32
    total = jnp.where(group == 0, value[0:rows], 0.0)
    for x in range(1, count):
        total = total + jnp.where(group == x, value[rows * x : rows * x + rows], 0.0)
    return total


def three(high, low, value):
    kept, rest = split(value)
    return dot(high, kept) + dot(high, rest) + dot(low, kept)


def solve(block_high, block_low, rows_ref):
    return own_lanes(three(block_high, block_low, rows_ref[...]))


def first_kernel(
    lower_ref, upper_ref, middle_ref, below_ref, above_ref, own_ref, left_ref, right_ref,
    g_ref, wide_ref, x_ref, bh_ref, bl_ref, rows,
):
    for z in range(2):
        rows[...] = jnp.zeros((32, 384), F32)
        node = lower_ref[z] + below_ref[z]
        top = upper_ref[z] + above_ref[z]
        middle = middle_ref[z]
        for slot, (source, at) in enumerate(((node, 0), (top, 0), (middle, 0), (node, 4), (top, 4))):
            rows[3 * slot : 3 * slot + 3] = source[at : at + 3] / source[at + 3 : at + 4]
        parts = [ref[z, 48:72, 32 * x : 32 * x + 32] for ref in (left_ref, own_ref, right_ref) for x in range(4)]
        high, low = split(jnp.concatenate(parts, axis=0))
        bh_ref[z], bl_ref[z] = high[48:240], low[48:240]
        found = by_x(three(high, low, rows[...]), 12, 24)
        x_ref[z] = jnp.where(lax.broadcasted_iota(jnp.int32, (16, 384), 0) < 15, found[0:16], 0.0)
        g_ref[z] = rows[0:16]
        wide_ref[z, 0:16] = pltpu.roll(rows[0:16], 320, 1)[:, 0:256]
        wide_ref[z, 15:24] = pltpu.roll(rows[0:16], 288, 1)[6:15, 0:256]


def merge_kernel(near_ref, far_ref, left_ref, right_ref, ah_ref, al_ref):
    for z in range(2):
        cells = [ref[x, z] for ref in (left_ref, near_ref, far_ref, right_ref) for x in range(2)]
        ah_ref[z], al_ref[z] = split(jnp.concatenate(cells, axis=0))


def views(near, far):
    lane = lanes(near.shape)
    return (
        pltpu.roll(jnp.where(lane >= 96, far, near), 32, 1),
        near,
        pltpu.roll(jnp.where(lane < 32, far, near), 96, 1),
        pltpu.roll(jnp.where(lane < 64, far, near), 64, 1),
    )


def product(high, low, kh_ref, kl_ref, z):
    kept = jnp.concatenate([h[48 * z : 48 * z + 192] for h in high], axis=0)
    rest = jnp.concatenate([h[48 * z : 48 * z + 192] for h in low], axis=0)
    both = dot(kh_ref[z], jnp.concatenate([kept, rest], axis=1))
    return own_lanes(both[:, 0:128] + both[:, 128:256] + dot(kl_ref[z], kept))


def gathered(odd_ref, own_ref, first_ref, second_ref):
    left, right = sides_of(odd_ref, first_ref, second_ref)
    all_z = jnp.concatenate([left, own_ref[0:96], right], axis=0)
    return views(all_z[:, 0:128], all_z[:, 128:256])


def layers_kernel(even_ref, x_ref, first_ref, second_ref, *rest):
    out_ref = rest[-1]
    even = jnp.full(x_ref.shape[1:], even_ref[0], jnp.int32) == 1
    for z in range(2):
        out_ref[48 * z : 48 * z + 16] = x_ref[z]
        out_ref[48 * z + 16 : 48 * z + 32] = jnp.where(even, first_ref[z], second_ref[z])
        out_ref[48 * z + 32 : 48 * z + 48] = jnp.where(even, second_ref[z], first_ref[z])
    if len(rest) == 2:
        out_ref[96:112] = rest[0][0]


def sides_of(odd_ref, first_ref, second_ref):
    odd = jnp.full(first_ref.shape, odd_ref[0], jnp.int32) == 1
    return jnp.where(odd[48:96], second_ref[48:96], first_ref[48:96]), jnp.where(odd, first_ref[...], second_ref[...])


def sweep_kernel(top, odd_ref, own_ref, first_ref, second_ref, g_ref, ah_ref, al_ref, bh_ref, bl_ref, x_ref, rows, closed):
    left, right = sides_of(odd_ref, first_ref, second_ref)
    seen = jnp.concatenate([left, own_ref[0:96], right[0:96]], axis=0)
    look = [pltpu.roll(seen, 384 - 32 * start, 1)[:, 0:256] for start in (1, 2, 3, 4)]
    pairs = [split(view) for view in look]
    rows[24:32] = jnp.zeros((8, 256), F32)
    for z in range(2):
        kept = jnp.concatenate([p[0][48 * z : 48 * z + 192] for p in pairs], axis=0)
        rest = jnp.concatenate([p[1][48 * z : 48 * z + 192] for p in pairs], axis=0)
        both = dot(ah_ref[z], jnp.concatenate([kept, rest], axis=1))
        found = by_x(both[:, 0:256] + both[:, 256:512] + dot(al_ref[z], kept), 8, 24)
        rows[0:24] = g_ref[z] - found
        found = by_x(three(bh_ref[z], bl_ref[z], rows[...]), 8, 24)
        rows[0:24] = found
        at = 48 * z + 48
        body_rows = look[1][at : at + 16] + rows[0:16]
        body_rows = jnp.where(lax.broadcasted_iota(jnp.int32, (16, 256), 0) < 15, body_rows, 0.0)
        closed[...] = jnp.zeros((16, 256), F32)
        closed[6:15] = rows[15:24]
        after = look[2][at : at + 16] + closed[...]
        row = lax.broadcasted_iota(jnp.int32, (16, 256), 0)
        after = jnp.where((row >= 6) & (row < 15), after, 0.0)
        if top == 5:
            pad = jnp.zeros((16, 128), F32)
            body_rows = pltpu.roll(jnp.concatenate([body_rows, pad], axis=1), 64, 1)
            after = pltpu.roll(jnp.concatenate([after, pad], axis=1), 96, 1)
            x_ref[z] = jnp.where(lanes((16, 384)) // 32 == 10, after, body_rows)
        else:
            after = pltpu.roll(after, 32, 1)
            use = (lanes((16, 256)) // 32 == 7) & (row >= 6)
            x_ref[z] = pltpu.roll(jnp.where(use, after, body_rows), 192, 1)


def average_kernel(odd_ref, g_ref, first_ref, second_ref, wide_ref, out_ref, ahead):
    for z in range(3):
        source = g_ref[z] if z < 2 else sides_of(odd_ref, first_ref, second_ref)[1][96:112]
        ahead[z, 0:16] = source[:, 128:256]
        ahead[z, 16:32] = views(source[:, 128:256], source[:, 256:384])[2]
    for z in range(2):
        wide_ref[z] = jnp.zeros((48, 128), F32)
        for edge in range(12):
            ox, _, oz = OFFSETS[edge]
            start = 16 * ox + 3 * slot_of(edge)
            value = ahead[z + oz, start : start + 3]
            wide_ref[z, 3 * edge : 3 * edge + 3] = value
        write(out_ref, z, wide_ref[z, 0:36])


def write(out_ref, z, value):
    for x in range(4):
        out_ref[x, z] = value[:, 32 * x : 32 * x + 32]


def last_kernel(
    odd_ref, own_ref, first_ref, second_ref, wide_ref, ah_ref, al_ref, bh_ref, bl_ref, out_ref, rows, ahead, state
):
    seen = gathered(odd_ref, own_ref, first_ref, second_ref)
    pairs = [split(view) for view in seen]
    high, low = [p[0] for p in pairs], [p[1] for p in pairs]
    state[...] = jnp.zeros((40, 128), F32)
    for z in range(3):
        ahead[z, 0:16] = seen[1][48 * z + 48 : 48 * z + 64]
        ahead[z, 16:32] = seen[2][48 * z + 48 : 48 * z + 64]
    for z in range(2):
        for edge in range(12):
            ox, _, oz = OFFSETS[edge]
            start = 16 * ox + 3 * slot_of(edge)
            state[3 * edge : 3 * edge + 3] = ahead[z + oz, start : start + 3]
        rows[...] = jnp.zeros((48, 128), F32)
        rows[0:36] = wide_ref[z, 0:36] - product(high, low, ah_ref, al_ref, z)[0:36]
        state[...] = state[...] + solve(bh_ref[z, :, 0:48], bl_ref[z, :, 0:48], rows)
        turned = state[...].T
        for x in range(4):
            out_ref[x, z] = turned[32 * x : 32 * x + 32, 0:36]


def after(value, *others):
    return lax.optimization_barrier((value, *others))[0]


def steps(displacement, dof_weight, coarse_matrix, block_inverse):
    weights = jnp.transpose(dof_weight[:, 0], (0, 2, 1, 3)).reshape(4, 24, 128)
    matrix = jnp.transpose(coarse_matrix[:, 0], (0, 2, 3, 1, 4)).reshape(4, 27, 72, 36)
    block = jnp.transpose(block_inverse[:, 0], (0, 2, 1, 3)).reshape(4, 72, 36)
    mine, ah, al, bh, bl, low_x, high_x = start(displacement[:, 0], weights, block, matrix)
    pair = []
    for which in range(2):
        pair.append(matched(mine, "gx", which))
    left, right = ordered(lax.axis_index("gx") % 2 == 0, pair)
    sides = (mine, left, right)
    sums, up = call(sum_x_kernel, (shape(2, 32, 384), shape(24, 384)))(*sides)
    left = shifted(up, "gz", 1)
    lower, upper, middle = call(sum_z_kernel, (shape(2, 8, 384),) * 3)(sums, left)
    even = lax.axis_index("gy") % 2 == 0
    even_row = even.astype(jnp.int32).reshape(1)
    odd = (lax.axis_index("gz") % 2).astype(jnp.int32).reshape(1)
    sent_down, sent_up = ordered(even, (lower, upper))
    pair = []
    for which, value in enumerate((sent_down, sent_up)):
        pair.append(matched(value, "gy", which))
    below, above = ordered(even, pair)
    rows_left = shifted(after(high_x, upper), "gx", 1)
    g, near, x, near_high, near_low = call(
        first_kernel,
        (shape(2, 16, 384), shape(2, 24, 256), shape(2, 16, 384)) + (shape(2, 192, 32, dtype=BF16),) * 2,
        (pltpu.VMEM((32, 384), F32),),
    )(lower, upper, middle, below, above, *sides)
    for sweep in range(3):
        pair = []
        for which in range(2):
            pair.append(matched(x, "gy", which))
        if sweep == 0:
            rows_right = shifted(after(low_x, x), "gx", -1)
            rows_right = after(rows_right, *pair)
            wide = (shape(2, 192, 768, dtype=BF16),) * 2
            operator = call(merge_kernel, wide, flops=10_000_000)(low_x, high_x, rows_left, rows_right)
        pieces = (x, *pair, g) if sweep == 0 else (x, *pair)
        rows = shape(112 if sweep == 0 else 96, x.shape[2])
        own = call(layers_kernel, rows, scalar=True, count=len(pieces))(even_row, *pieces)
        pair = []
        for which in range(2):
            pair.append(matched(own, "gz", which))
        if sweep == 0:
            every, average = call(
                average_kernel,
                (shape(2, 48, 128), shape(4, 2, 36, 32)),
                (pltpu.VMEM((3, 32, 128), F32),),
                scalar=True,
                count=3,
            )(odd, g, *pair)
        if sweep < 2:
            x = call(
                functools.partial(sweep_kernel, 5 - sweep),
                shape(2, 16, 384 if sweep == 0 else 256),
                (pltpu.VMEM((32, 256), F32), pltpu.VMEM((16, 256), F32)),
                flops=20_000_000,
                scalar=True,
                count=8,
            )(odd, own, *pair, near, *operator, near_high, near_low)
    x = call(
        last_kernel,
        shape(4, 2, 32, 36),
        (pltpu.VMEM((48, 128), F32), pltpu.VMEM((3, 32, 128), F32), pltpu.VMEM((40, 128), F32)),
        flops=10_000_000,
        scalar=True,
        count=8,
    )(odd, own, *pair, every, ah, al, bh, bl)
    return average.reshape(4, 1, 2, 12, 3, 32), jnp.swapaxes(x, 2, 3)[:, None]


def solution(mesh):
    placed = (
        P("gx", "gy", "gz", None, None, None, None),
        P("gx", "gy", "gz", None, None),
        P("gx", "gy", "gz", None, None, None),
        P("gx", "gy", "gz", None, None),
    )
    return jax.shard_map(
        steps,
        mesh=mesh,
        in_specs=placed,
        out_specs=(P("gx", "gy", "gz", None, None, None), P("gx", "gy", "gz", None, None)),
        check_vma=False,
    )
```

```python
import functools

import jax
import jax.numpy as jnp
import numpy as np
from jax import lax
from jax.experimental import pallas as pl
from jax.experimental.pallas import tpu as pltpu
from jax.sharding import PartitionSpec as P


F32 = jnp.float32
BF16 = jnp.bfloat16
OFFSETS = (
    (0, 0, 0), (0, 0, 1), (0, 1, 0), (0, 1, 1),
    (0, 0, 0), (0, 0, 1), (1, 0, 0), (1, 0, 1),
    (0, 0, 0), (0, 1, 0), (1, 0, 0), (1, 1, 0),
)
WIDE_EDGES = (0, 2, 4, 8, 9, 6, 10, 11)


def slot_of(edge):
    direction = edge // 4
    upper = OFFSETS[edge][1]
    return (0 + upper, 2, 3 + upper)[direction]


def placement():
    table = np.zeros((384, 384), np.float32)
    for offset in range(9):
        dy, dz = offset // 3 - 1, offset % 3 - 1
        for edge in range(12):
            ox, oy, oz = OFFSETS[edge]
            direction = edge // 4
            if direction == 1:
                group, slot = {-1: (1, 2), 0: (0, 2), 1: (2, 2)}[dy + oy]
            else:
                base = 0 if direction == 0 else 3
                group, slot = {-1: (1, base), 0: (0, base), 1: (0, base + 1), 2: (2, base + 1)}[dy + oy]
            for comp in range(3):
                row = 16 * group + 3 * slot + comp
                table[36 * offset + 3 * edge + comp, 192 * ox + 48 * (dz + oz + 1) + row] = 1.0
    return table


def choice():
    table = np.zeros((512, 128), np.float32)
    for x in range(4):
        for place, edge in enumerate(WIDE_EDGES):
            for comp in range(3):
                table[128 * x + 3 * edge + comp, 32 * x + 3 * place + comp] = 1.0
    return table


def shifted(block, axis, distance):
    count = lax.axis_size(axis)
    return lax.ppermute(block, axis, [((i - distance) % count, i) for i in range(count)])


def matched(block, axis, which):
    count = lax.axis_size(axis)
    return lax.ppermute(block, axis, [(i, (i - 1 if i % 2 == which else i + 1) % count) for i in range(count)])


def ordered(even, pair):
    return jnp.where(even, pair[0], pair[1]), jnp.where(even, pair[1], pair[0])


def lanes(shape):
    return lax.broadcasted_iota(jnp.int32, shape, len(shape) - 1)


def split(value):
    high = value.astype(BF16)
    return high, (value - high.astype(F32)).astype(BF16)


def dot(a, b):
    return jnp.dot(a, b, preferred_element_type=F32)


def own_lanes(value):
    group = lanes((40, 128)) // 32
    total = jnp.where(group == 0, value[0:40], 0.0)
    for x in range(1, 4):
        total = total + jnp.where(group == x, value[40 * x : 40 * x + 40], 0.0)
    return total


def call(kernel, outs, scratch=(), flops=1_000_000, scalar=False, count=0, **options):
    if scalar:
        places = [pltpu.SMEM] + [pltpu.VMEM] * count
        options["in_specs"] = [pl.BlockSpec(memory_space=place) for place in places]
    return pl.pallas_call(
        kernel,
        out_shape=outs,
        scratch_shapes=list(scratch),
        cost_estimate=pl.CostEstimate(flops=flops, bytes_accessed=1_000_000, transcendentals=0),
        compiler_params=pltpu.CompilerParams(vmem_limit_bytes=40 * 1024 * 1024),
        **options,
    )


def streamed(*arrays):
    return [pltpu.with_memory_space_constraint(a, pltpu.HBM) for a in arrays]


def shape(*dims, dtype=F32):
    return jax.ShapeDtypeStruct(dims, dtype)


def take_sums(step, disp_ref, weights, held):
    ones = jnp.ones((128, 128), BF16)
    group = (lanes((4, 512)) % 128) // 32
    keep = group == lax.broadcasted_iota(jnp.int32, (4, 512), 0)
    for z in range(2):
        pieces = []
        for edge in range(3):
            parts = [disp_ref[x, z, edge, c] for c in range(3) for x in range(4)]
            right = jnp.concatenate(parts + [ones], axis=0)
            at = 6 * step + 2 * edge + z
            left = jnp.concatenate([weights[x, pl.ds(at, 1), :] for x in range(4)], axis=0).astype(BF16)
            found = lax.dot_general(left, right, (((1,), (1,)), ((), ())), preferred_element_type=F32)
            row = jnp.sum(jnp.where(keep, found, 0.0), axis=0, keepdims=True)
            pieces = pieces + [row[:, 128 * c : 128 * c + 128] for c in range(4)]
        held[step, z, 0:12] = jnp.concatenate(pieces, axis=0)


def take_operator(step, matrix_ref, place_ref, ah_ref, al_ref, halves, packed, stacked, full):
    for offset in range(27):
        start, tile = 36 * (offset % 9) % 128, 3 * (offset // 9) + 36 * (offset % 9) // 128
        size = min(36, 128 - start)
        packed[tile, :, start : start + size] = matrix_ref[0, offset, :, 0:size]
        if size < 36:
            packed[tile + 1, :, 0 : 36 - size] = matrix_ref[0, offset, :, size:36]
    pad = jnp.zeros((4, 384), BF16)
    found = []
    for dx in range(3):
        for z in range(2):
            high, low = split(
                jnp.concatenate([packed[3 * dx + k, pl.ds(z, 36, stride=2), :] for k in range(3)], axis=1)
            )
            stacked[40 * z : 40 * z + 40] = jnp.concatenate([high, pad], axis=0)
            stacked[80 + 40 * z : 120 + 40 * z] = jnp.concatenate([low, pad], axis=0)
        found.append(dot(stacked[...], place_ref[...]))
    none = jnp.zeros((160, 384), F32)
    total = jnp.concatenate([found[0], found[2]], axis=1)
    total = total + pltpu.roll(jnp.concatenate([found[1], none], axis=1), 192, 1)
    for z in range(2):
        high, low = total[40 * z : 40 * z + 40], total[80 + 40 * z : 120 + 40 * z]
        ah_ref[z, 0] = high.astype(BF16)
        al_ref[z, 0] = low.astype(BF16)
        full[...] = high + low
        for half, half_ref in enumerate(halves):

            @pl.when(step // 2 == half)
            def _(half_ref=half_ref, z=z):
                for place, edge in enumerate(WIDE_EDGES):
                    half_ref[0, z, 3 * place : 3 * place + 3] = full[3 * edge : 3 * edge + 3]


def start_kernel(
    disp_ref, weight_ref, block_ref, choice_ref, matrix_ref, place_ref,
    sums_ref, ah_ref, al_ref, bh_ref, bl_ref, near_ref, far_ref,
    weights, inner, rows, held, packed, stacked, full,
):
    step = pl.program_id(0)

    @pl.when(step == 0)
    def _():
        weights[...] = weight_ref[...].astype(F32)
        inner[...] = jnp.zeros((4, 72, 128), F32)
        for tile in range(9):
            packed[tile] = jnp.zeros((72, 128), F32)
        for x in range(4):
            inner[x, :, 0:36] = block_ref[x]
        for z in range(2):
            value = jnp.concatenate([inner[x, pl.ds(z, 36, stride=2), :] for x in range(4)], axis=1)
            high, low = split(value)
            rows[0:36] = dot(high, choice_ref[...]) + dot(low, choice_ref[...])
            for place, edge in enumerate(WIDE_EDGES):
                sums_ref[z, 48 + 3 * place : 51 + 3 * place] = rows[3 * edge : 3 * edge + 3]

    take_sums(step, disp_ref, weights, held)
    take_operator(step, matrix_ref, place_ref, ah_ref, al_ref, (near_ref, far_ref), packed, stacked, full)
    for z in range(2):
        high, low = split(inner[step, pl.ds(z, 36, stride=2), :])
        pad = jnp.zeros((4, 128), BF16)
        bh_ref[z, 0] = jnp.concatenate([high, pad], axis=0)
        bl_ref[z, 0] = jnp.concatenate([low, pad], axis=0)

    @pl.when(step == 3)
    def _():
        for z in range(2):
            for part in range(4):
                sums_ref[z, 12 * part : 12 * part + 12] = held[part, z, 0:12]


def start(displacement, weights, block, matrix):
    outs = (shape(2, 72, 128),) + (shape(2, 4, 40, 768, dtype=BF16),) * 2
    outs = outs + (shape(2, 4, 40, 128, dtype=BF16),) * 2 + (shape(2, 2, 24, 768),) * 2
    wide = pl.BlockSpec((2, 1, 40, 768), lambda i: (0, i, 0, 0))
    slim = pl.BlockSpec((2, 1, 40, 128), lambda i: (0, i, 0, 0))
    sums, ah, al, bh, bl, near, far = call(
        start_kernel,
        outs,
        (
            pltpu.VMEM((4, 24, 128), F32),
            pltpu.VMEM((4, 72, 128), F32),
            pltpu.VMEM((40, 128), F32),
            pltpu.VMEM((4, 2, 16, 128), F32),
            pltpu.VMEM((9, 72, 128), F32),
            pltpu.VMEM((160, 384), BF16),
            pltpu.VMEM((40, 768), F32),
        ),
        flops=40_000_000,
        grid=(4,),
        in_specs=[
            pl.BlockSpec((4, 2, 3, 3, 32, 128), lambda i: (0, 0, i, 0, 0, 0)),
            pl.BlockSpec((4, 24, 128), lambda i: (0, 0, 0)),
            pl.BlockSpec((4, 72, 36), lambda i: (0, 0, 0)),
            pl.BlockSpec((512, 128), lambda i: (0, 0)),
            pl.BlockSpec((1, 27, 72, 36), lambda i: (i, 0, 0, 0)),
            pl.BlockSpec((384, 384), lambda i: (0, 0)),
        ],
        out_specs=(
            pl.BlockSpec((2, 72, 128), lambda i: (0, 0, 0)),
            wide,
            wide,
            slim,
            slim,
            pl.BlockSpec((1, 2, 24, 768), lambda i: (jnp.minimum(i, 1), 0, 0, 0)),
            pl.BlockSpec((1, 2, 24, 768), lambda i: (jnp.maximum(i - 2, 0), 0, 0, 0)),
        ),
    )(*streamed(displacement, weights, block, jnp.asarray(choice(), BF16), matrix, jnp.asarray(placement(), BF16)))
    return (
        sums, ah.reshape(2, 160, 768), al.reshape(2, 160, 768),
        bh.reshape(2, 160, 128), bl.reshape(2, 160, 128), near, far,
    )


def sum_x_kernel(sums_ref, left_ref, right_ref, out_ref, up_ref):
    for z in range(2):
        all_x = jnp.concatenate([left_ref[z, 0:48], sums_ref[z, 0:48], right_ref[z, 0:48]], axis=1)
        below = pltpu.roll(all_x, 32, 1)
        out_ref[z, 0:16] = all_x[0:16]
        out_ref[z, 16:24] = all_x[16:24] + below[24:32]
        out_ref[z, 24:32] = all_x[32:40] + below[40:48]
    up_ref[...] = out_ref[1, 0:24]


def sum_z_kernel(sums_ref, left_ref, lower_ref, upper_ref, middle_ref):
    for z in range(2):
        below = left_ref if z == 0 else sums_ref.at[0]
        lower_ref[z, 0:4] = sums_ref[z, 0:4] + below[4:8]
        lower_ref[z, 4:8] = sums_ref[z, 24:28]
        upper_ref[z, 0:4] = sums_ref[z, 8:12] + below[12:16]
        upper_ref[z, 4:8] = sums_ref[z, 28:32]
        middle_ref[z, 0:4] = sums_ref[z, 16:20] + below[20:24]
        middle_ref[z, 4:8] = sums_ref[z, 16:20]


def by_x(value, count, rows):
    group = lanes((rows, value.shape[1])) // 32
    total = jnp.where(group == 0, value[0:rows], 0.0)
    for x in range(1, count):
        total = total + jnp.where(group == x, value[rows * x : rows * x + rows], 0.0)
    return total


def three(high, low, value):
    kept, rest = split(value)
    return dot(high, kept) + dot(high, rest) + dot(low, kept)


def solve(block_high, block_low, rows_ref):
    return own_lanes(three(block_high, block_low, rows_ref[...]))


def first_kernel(
    lower_ref, upper_ref, middle_ref, below_ref, above_ref, own_ref, left_ref, right_ref,
    g_ref, wide_ref, x_ref, bh_ref, bl_ref, rows,
):
    for z in range(2):
        rows[...] = jnp.zeros((32, 384), F32)
        node = lower_ref[z] + below_ref[z]
        top = upper_ref[z] + above_ref[z]
        middle = middle_ref[z]
        for slot, (source, at) in enumerate(((node, 0), (top, 0), (middle, 0), (node, 4), (top, 4))):
            rows[3 * slot : 3 * slot + 3] = source[at : at + 3] / source[at + 3 : at + 4]
        parts = [ref[z, 48:72, 32 * x : 32 * x + 32] for ref in (left_ref, own_ref, right_ref) for x in range(4)]
        high, low = split(jnp.concatenate(parts, axis=0))
        bh_ref[z], bl_ref[z] = high[48:240], low[48:240]
        found = by_x(three(high, low, rows[...]), 12, 24)
        x_ref[z] = jnp.where(lax.broadcasted_iota(jnp.int32, (16, 384), 0) < 15, found[0:16], 0.0)
        g_ref[z] = rows[0:16]
        wide_ref[z, 0:16] = pltpu.roll(rows[0:16], 320, 1)[:, 0:256]
        wide_ref[z, 15:24] = pltpu.roll(rows[0:16], 288, 1)[6:15, 0:256]


def merge_kernel(near_ref, far_ref, left_ref, right_ref, ah_ref, al_ref):
    for z in range(2):
        cells = [ref[x, z] for ref in (left_ref, near_ref, far_ref, right_ref) for x in range(2)]
        ah_ref[z], al_ref[z] = split(jnp.concatenate(cells, axis=0))


def views(near, far):
    lane = lanes(near.shape)
    return (
        pltpu.roll(jnp.where(lane >= 96, far, near), 32, 1),
        near,
        pltpu.roll(jnp.where(lane < 32, far, near), 96, 1),
        pltpu.roll(jnp.where(lane < 64, far, near), 64, 1),
    )


def product(high, low, kh_ref, kl_ref, z):
    kept = jnp.concatenate([h[48 * z : 48 * z + 192] for h in high], axis=0)
    rest = jnp.concatenate([h[48 * z : 48 * z + 192] for h in low], axis=0)
    both = dot(kh_ref[z], jnp.concatenate([kept, rest], axis=1))
    return own_lanes(both[:, 0:128] + both[:, 128:256] + dot(kl_ref[z], kept))


def gathered(odd_ref, own_ref, first_ref, second_ref):
    left, right = sides_of(odd_ref, first_ref, second_ref)
    all_z = jnp.concatenate([left, own_ref[0:96], right], axis=0)
    return views(all_z[:, 0:128], all_z[:, 128:256])


def layers_kernel(even_ref, x_ref, first_ref, second_ref, *rest):
    out_ref = rest[-1]
    even = jnp.full(x_ref.shape[1:], even_ref[0], jnp.int32) == 1
    for z in range(2):
        out_ref[48 * z : 48 * z + 16] = x_ref[z]
        out_ref[48 * z + 16 : 48 * z + 32] = jnp.where(even, first_ref[z], second_ref[z])
        out_ref[48 * z + 32 : 48 * z + 48] = jnp.where(even, second_ref[z], first_ref[z])
    if len(rest) == 2:
        out_ref[96:112] = rest[0][0]


def sides_of(odd_ref, first_ref, second_ref):
    odd = jnp.full(first_ref.shape, odd_ref[0], jnp.int32) == 1
    return jnp.where(odd[48:96], second_ref[48:96], first_ref[48:96]), jnp.where(odd, first_ref[...], second_ref[...])


def sweep_kernel(top, odd_ref, own_ref, first_ref, second_ref, g_ref, ah_ref, al_ref, bh_ref, bl_ref, x_ref, rows, closed):
    left, right = sides_of(odd_ref, first_ref, second_ref)
    seen = jnp.concatenate([left, own_ref[0:96], right[0:96]], axis=0)
    look = [pltpu.roll(seen, 384 - 32 * start, 1)[:, 0:256] for start in (1, 2, 3, 4)]
    pairs = [split(view) for view in look]
    rows[24:32] = jnp.zeros((8, 256), F32)
    for z in range(2):
        kept = jnp.concatenate([p[0][48 * z : 48 * z + 192] for p in pairs], axis=0)
        rest = jnp.concatenate([p[1][48 * z : 48 * z + 192] for p in pairs], axis=0)
        both = dot(jnp.concatenate([ah_ref[z], al_ref[z]], axis=0), kept)
        found = by_x(both[0:192] + both[192:384] + dot(ah_ref[z], rest), 8, 24)
        rows[0:24] = g_ref[z] - found
        found = by_x(three(bh_ref[z], bl_ref[z], rows[...]), 8, 24)
        rows[0:24] = found
        at = 48 * z + 48
        body_rows = look[1][at : at + 16] + rows[0:16]
        body_rows = jnp.where(lax.broadcasted_iota(jnp.int32, (16, 256), 0) < 15, body_rows, 0.0)
        closed[...] = jnp.zeros((16, 256), F32)
        closed[6:15] = rows[15:24]
        after = look[2][at : at + 16] + closed[...]
        row = lax.broadcasted_iota(jnp.int32, (16, 256), 0)
        after = jnp.where((row >= 6) & (row < 15), after, 0.0)
        if top == 5:
            pad = jnp.zeros((16, 128), F32)
            body_rows = pltpu.roll(jnp.concatenate([body_rows, pad], axis=1), 64, 1)
            after = pltpu.roll(jnp.concatenate([after, pad], axis=1), 96, 1)
            x_ref[z] = jnp.where(lanes((16, 384)) // 32 == 10, after, body_rows)
        else:
            after = pltpu.roll(after, 32, 1)
            use = (lanes((16, 256)) // 32 == 7) & (row >= 6)
            x_ref[z] = pltpu.roll(jnp.where(use, after, body_rows), 192, 1)


def average_kernel(odd_ref, g_ref, first_ref, second_ref, wide_ref, out_ref, ahead):
    for z in range(3):
        source = g_ref[z] if z < 2 else sides_of(odd_ref, first_ref, second_ref)[1][96:112]
        ahead[z, 0:16] = source[:, 128:256]
        ahead[z, 16:32] = views(source[:, 128:256], source[:, 256:384])[2]
    for z in range(2):
        wide_ref[z] = jnp.zeros((48, 128), F32)
        for edge in range(12):
            ox, _, oz = OFFSETS[edge]
            start = 16 * ox + 3 * slot_of(edge)
            value = ahead[z + oz, start : start + 3]
            wide_ref[z, 3 * edge : 3 * edge + 3] = value
        write(out_ref, z, wide_ref[z, 0:36])


def write(out_ref, z, value):
    for x in range(4):
        out_ref[x, z] = value[:, 32 * x : 32 * x + 32]


def last_kernel(
    odd_ref, own_ref, first_ref, second_ref, wide_ref, ah_ref, al_ref, bh_ref, bl_ref, out_ref, rows, ahead, state
):
    seen = gathered(odd_ref, own_ref, first_ref, second_ref)
    pairs = [split(view) for view in seen]
    high, low = [p[0] for p in pairs], [p[1] for p in pairs]
    state[...] = jnp.zeros((40, 128), F32)
    for z in range(3):
        ahead[z, 0:16] = seen[1][48 * z + 48 : 48 * z + 64]
        ahead[z, 16:32] = seen[2][48 * z + 48 : 48 * z + 64]
    for z in range(2):
        for edge in range(12):
            ox, _, oz = OFFSETS[edge]
            start = 16 * ox + 3 * slot_of(edge)
            state[3 * edge : 3 * edge + 3] = ahead[z + oz, start : start + 3]
        rows[...] = jnp.zeros((48, 128), F32)
        rows[0:36] = wide_ref[z, 0:36] - product(high, low, ah_ref, al_ref, z)[0:36]
        state[...] = state[...] + solve(bh_ref[z, :, 0:48], bl_ref[z, :, 0:48], rows)
        turned = state[...].T
        for x in range(4):
            out_ref[x, z] = turned[32 * x : 32 * x + 32, 0:36]


def after(value, *others):
    return lax.optimization_barrier((value, *others))[0]


def steps(displacement, dof_weight, coarse_matrix, block_inverse):
    weights = jnp.transpose(dof_weight[:, 0], (0, 2, 1, 3)).reshape(4, 24, 128)
    matrix = jnp.transpose(coarse_matrix[:, 0], (0, 2, 3, 1, 4)).reshape(4, 27, 72, 36)
    block = jnp.transpose(block_inverse[:, 0], (0, 2, 1, 3)).reshape(4, 72, 36)
    mine, ah, al, bh, bl, low_x, high_x = start(displacement[:, 0], weights, block, matrix)
    pair = []
    for which in range(2):
        pair.append(matched(mine, "gx", which))
    left, right = ordered(lax.axis_index("gx") % 2 == 0, pair)
    sides = (mine, left, right)
    sums, up = call(sum_x_kernel, (shape(2, 32, 384), shape(24, 384)))(*sides)
    left = shifted(up, "gz", 1)
    lower, upper, middle = call(sum_z_kernel, (shape(2, 8, 384),) * 3)(sums, left)
    even = lax.axis_index("gy") % 2 == 0
    even_row = even.astype(jnp.int32).reshape(1)
    odd = (lax.axis_index("gz") % 2).astype(jnp.int32).reshape(1)
    sent_down, sent_up = ordered(even, (lower, upper))
    pair = []
    for which, value in enumerate((sent_down, sent_up)):
        pair.append(matched(value, "gy", which))
    below, above = ordered(even, pair)
    rows_left = shifted(after(high_x, upper), "gx", 1)
    g, near, x, near_high, near_low = call(
        first_kernel,
        (shape(2, 16, 384), shape(2, 24, 256), shape(2, 16, 384)) + (shape(2, 192, 32, dtype=BF16),) * 2,
        (pltpu.VMEM((32, 384), F32),),
    )(lower, upper, middle, below, above, *sides)
    for sweep in range(3):
        pair = []
        for which in range(2):
            pair.append(matched(x, "gy", which))
        if sweep == 0:
            rows_right = shifted(after(low_x, x), "gx", -1)
            rows_right = after(rows_right, *pair)
            wide = (shape(2, 192, 768, dtype=BF16),) * 2
            operator = call(merge_kernel, wide, flops=10_000_000)(low_x, high_x, rows_left, rows_right)
        if sweep == 1:
            pair[0] = after(pair[0], every)
        pieces = (x, *pair, g) if sweep == 0 else (x, *pair)
        rows = shape(112 if sweep == 0 else 96, x.shape[2])
        own = call(layers_kernel, rows, scalar=True, count=len(pieces))(even_row, *pieces)
        pair = []
        for which in range(2):
            pair.append(matched(own, "gz", which))
        if sweep == 0:
            every, average = call(
                average_kernel,
                (shape(2, 48, 128), shape(4, 2, 36, 32)),
                (pltpu.VMEM((3, 32, 128), F32),),
                scalar=True,
                count=3,
            )(odd, g, *pair)
        if sweep < 2:
            x = call(
                functools.partial(sweep_kernel, 5 - sweep),
                shape(2, 16, 384 if sweep == 0 else 256),
                (pltpu.VMEM((32, 256), F32), pltpu.VMEM((16, 256), F32)),
                flops=20_000_000,
                scalar=True,
                count=8,
            )(odd, own, *pair, near, *operator, near_high, near_low)
    x = call(
        last_kernel,
        shape(4, 2, 32, 36),
        (pltpu.VMEM((48, 128), F32), pltpu.VMEM((3, 32, 128), F32), pltpu.VMEM((40, 128), F32)),
        flops=10_000_000,
        scalar=True,
        count=8,
    )(odd, own, *pair, every, ah, al, bh, bl)
    return average.reshape(4, 1, 2, 12, 3, 32), jnp.swapaxes(x, 2, 3)[:, None]


def solution(mesh):
    placed = (
        P("gx", "gy", "gz", None, None, None, None),
        P("gx", "gy", "gz", None, None),
        P("gx", "gy", "gz", None, None, None),
        P("gx", "gy", "gz", None, None),
    )
    return jax.shard_map(
        steps,
        mesh=mesh,
        in_specs=placed,
        out_specs=(P("gx", "gy", "gz", None, None, None), P("gx", "gy", "gz", None, None)),
        check_vma=False,
    )
```
